32 devices in a mesh: inner: 4 (over z), outer: 8 (over y, x, core).
Axes of the slice: x: 2, y: 2, z: 4, core: 2. Of those that a mesh axis runs over, the one named last changes fastest.
Arguments:
- inputs: bfloat16 [16, 1024, 2048], P('outer', 'inner'), may hold values from -6 to 6
- attn_gain: bfloat16 [2048], P(('inner', 'outer')), may hold values from 0.25 to 1.75
- w_query: bfloat16 [2048, 1536], P(('inner', 'outer')), may hold values from -0.125 to 0.125
- key_weight: bfloat16 [2048, 384], P(('inner', 'outer')), may hold values from -0.125 to 0.125
- value_weight: bfloat16 [2048, 384], P(('inner', 'outer')), may hold values from -0.125 to 0.125
- qk_gain: bfloat16 [128], P(('inner', 'outer')), may hold values from 1 to 2
- w_out: bfloat16 [1536, 2048], P(('inner', 'outer')), may hold values from -0.875 to 0.875
- ffn_gain: bfloat16 [2048], P(('inner', 'outer')), may hold values from 0.25 to 1.75
- w_gate: bfloat16 [2048, 4864], P(('inner', 'outer')), may hold values from -0.125 to 0.125
- w_up: bfloat16 [2048, 4864], P(('inner', 'outer')), may hold values from -0.125 to 0.125
- w_down: bfloat16 [4864, 2048], P(('inner', 'outer')), may hold values from -0.078125 to 0.078125
- cotangent: bfloat16 [16, 1024, 2048], P('outer', 'inner'), may hold values from -6 to 6
Outputs:
- result: bfloat16 [16, 1024, 2048], P('outer', 'inner')
- d_inputs: float32 [16, 1024, 2048], P('outer', 'inner')
- d_attn_gain: float32 [2048], P(('inner', 'outer'))
- d_query: float32 [2048, 1536], P(('inner', 'outer'))
- d_key: float32 [2048, 384], P(('inner', 'outer'))
- d_value: float32 [2048, 384], P(('inner', 'outer'))
- d_qk_gain: float32 [128], P(('inner', 'outer'))
- d_out: float32 [1536, 2048], P(('inner', 'outer'))
- d_ffn_gain: float32 [2048], P(('inner', 'outer'))
- d_gate: float32 [2048, 4864], P(('inner', 'outer'))
- d_up: float32 [2048, 4864], P(('inner', 'outer'))
- d_down: float32 [4864, 2048], P(('inner', 'outer'))
The draws below stay inside these ranges and needn't reach their ends.
All inputs are finite; a program needn't handle non-finite values.
Results may differ from the reference program's by a relative error of at most 0.025.
Values may be sent and summed in bfloat16 or wider, within the bound.
No kernel may reach another device: no remote copies, remote signals or barrier semaphores. Data moves between devices by JAX's collectives and lax.ppermute only.
A program may use at most 320 MiB of HBM per device.

```python
import jax
import jax.numpy as jnp
from jax import lax

MODEL_WIDTH = 2048
QUERY_HEADS = 24
KEY_VALUE_HEADS = 6
HEAD_SIZE = 64
FF = 4864
SEQUENCE_TOKENS = 1024
BLOCK = 256
SEQS = 2
SEQS_ALL = 16
N_OUTER = 8


def with_spikes(drawn, key, source, target, shards_of, factor):
    owner, partner = [(jnp.arange(drawn.shape[axis_at]) // (drawn.shape[axis_at] // shards_of)).reshape([-1 if axis == axis_at else 1 for axis in range(drawn.ndim)]) for axis_at in (source, target)]
    chosen = jax.random.permutation(key, shards_of)[partner]
    strong = (owner == chosen) | (owner == (partner + shards_of // 2) % shards_of)
    return jnp.where(strong, factor * drawn, drawn)


def steps_of(own_key, shape, shards, least, top_value):
    factor_of = 1.0
    for axis_at, parts in shards:
        steps = jax.random.uniform(jax.random.fold_in(jax.random.fold_in(own_key, 6), axis_at), (parts,), jnp.float32, least / len(shards), top_value / len(shards))
        factor_of = factor_of * jnp.repeat(jnp.exp(steps), shape[axis_at] // parts).reshape((-1,) + (1,) * (len(shape) - 1 - axis_at))
    return factor_of


def bell_draw(key, extent, spread, limit, cuts=(), held_as=jnp.bfloat16):
    values = jax.random.normal(key, extent, jnp.float32) * spread
    if len(cuts) > 0:
        values = steps_of(key, extent, cuts, -0.22, 0.18) * values
    return jnp.clip(values, min=-limit, max=limit).astype(held_as)


def bell_draw_with(key, dims, deviation, bound, shards, heavy, held_as=jnp.bfloat16):
    array = deviation * jax.random.normal(key, dims, jnp.float32)
    if shards:
        array = array * steps_of(key, dims, shards, -0.22, 0.18)
    return jnp.clip(with_spikes(array, jax.random.fold_in(key, 3), *heavy), -bound, bound).astype(held_as)


def setup_inputs(seed: int = 0) -> dict:
    seeds = jax.random.split(jax.random.key(seed), 13)
    inputs = bell_draw_with(seeds[0], (SEQS_ALL, SEQUENCE_TOKENS, MODEL_WIDTH), 1.0, 6.0, ((0, 8), (1, 4)), (0, 2, 8, 2.0))
    attn_gain = jnp.clip(1.0 + 0.15 * jax.random.normal(seeds[1], (MODEL_WIDTH,), jnp.float32), 0.25, 1.75).astype(jnp.bfloat16)
    w_query = bell_draw(seeds[2], (MODEL_WIDTH, QUERY_HEADS * HEAD_SIZE), MODEL_WIDTH ** -0.5, 0.125, ((0, 32),))
    key_weight = bell_draw(seeds[3], (MODEL_WIDTH, KEY_VALUE_HEADS * HEAD_SIZE), MODEL_WIDTH ** -0.5, 0.125, ((0, 32),))
    value_weight = bell_draw(seeds[4], (MODEL_WIDTH, KEY_VALUE_HEADS * HEAD_SIZE), MODEL_WIDTH ** -0.5, 0.125, ((0, 32),))
    qk_gain = jnp.clip(1.0 + 1.0 * jax.random.uniform(seeds[5], (2 * HEAD_SIZE,), jnp.float32) ** steps_of(seeds[5], (2 * HEAD_SIZE,), ((0, 32),), -0.2, 0.2), 1.0, 2.0).astype(jnp.bfloat16)
    w_out = bell_draw(seeds[6], (QUERY_HEADS * HEAD_SIZE, MODEL_WIDTH), (QUERY_HEADS * HEAD_SIZE // 32) ** -0.5, 0.875, ((0, 32),))
    ffn_gain = jnp.clip(1.0 + 0.15 * jax.random.normal(seeds[7], (MODEL_WIDTH,), jnp.float32), 0.25, 1.75).astype(jnp.bfloat16)
    w_gate = bell_draw(seeds[8], (MODEL_WIDTH, FF), MODEL_WIDTH ** -0.5, 0.125, ((0, 32),))
    w_up = bell_draw(seeds[9], (MODEL_WIDTH, FF), MODEL_WIDTH ** -0.5, 0.125, ((0, 32),))
    w_down = bell_draw(seeds[10], (FF, MODEL_WIDTH), FF ** -0.5, 0.078125, ((0, 32),))
    cotangent = bell_draw(seeds[11], (SEQS_ALL, SEQUENCE_TOKENS, MODEL_WIDTH), 1.0, 6.0, ((0, 8), (1, 4)))
    return {"inputs": inputs, "attn_gain": attn_gain, "w_query": w_query, "key_weight": key_weight, "value_weight": value_weight, "qk_gain": qk_gain, "w_out": w_out, "ffn_gain": ffn_gain, "w_gate": w_gate, "w_up": w_up, "w_down": w_down, "cotangent": cotangent}


EPS = 1e-06

@jax.custom_vjp
def lower_precision(v):
    return lax.optimization_barrier(v.astype(jnp.bfloat16)).astype(jnp.float32)

@jax.custom_vjp
def lower_precision_backward(v):
    return v

def low_keep(v):
    return (lower_precision(v), None)

def low_pass(kept, grad):
    return (grad,)

def back_keep(v):
    return (v, None)

def back_low(kept, grad):
    return (lower_precision(grad),)
lower_precision.defvjp(low_keep, low_pass)
lower_precision_backward.defvjp(back_keep, back_low)

def matrix_product(left, right):
    return jnp.einsum('...d,df->...f', left, right, precision=lax.Precision.HIGHEST)

def rms_norm(v, gain):
    return v * lax.rsqrt(lax.optimization_barrier(jnp.mean(v * v, axis=-1, keepdims=True)) + EPS) * gain

def tables(length):
    half = HEAD_SIZE // 2
    freq = 10000.0 ** (-jnp.arange(half, dtype=jnp.float32) * 2.0 / HEAD_SIZE)
    angle = jnp.arange(length, dtype=jnp.float32)[:, None] * freq[None, :]
    cosine_table = jnp.concatenate([jnp.cos(angle), jnp.cos(angle)], axis=-1)
    sine_table = jnp.concatenate([jnp.sin(angle), jnp.sin(angle)], axis=-1)
    return (cosine_table[None, :, None, :], sine_table[None, :, None, :])

def rotary_apply(v, cosine_table, sine_table):
    half = HEAD_SIZE // 2
    turned = jnp.concatenate([-v[..., half:], v[..., :half]], axis=-1)
    return v * cosine_table + turned * sine_table

def attend(query_rows, key, value_rows):
    batch_inputs, length = (query_rows.shape[0], query_rows.shape[1])
    token_rows = min(512, length)
    block_list = length // token_rows
    head_groups = QUERY_HEADS // KEY_VALUE_HEADS
    grouped_heads = query_rows.reshape(batch_inputs, block_list, token_rows, KEY_VALUE_HEADS, head_groups, HEAD_SIZE).transpose(1, 0, 2, 3, 4, 5)
    key_block = jnp.arange(length) // BLOCK

    def one_block(pair):
        piece, index = pair
        scores = jnp.einsum('bqhgd,bkhd->bhgqk', piece, key, precision=lax.Precision.HIGHEST) * HEAD_SIZE ** (-0.5)
        scores = lower_precision_backward(scores)
        query_block = (index * token_rows + jnp.arange(token_rows)) // BLOCK
        allowed = key_block[None, :] <= query_block[:, None]
        scores = jnp.where(allowed, scores, -1e+30)
        prob = lower_precision(jax.nn.softmax(scores, axis=-1))
        return jnp.einsum('bhgqk,bkhd->bqhgd', prob, value_rows, precision=lax.Precision.HIGHEST)
    mixed = lax.map(jax.checkpoint(one_block), (grouped_heads, jnp.arange(block_list)))
    return mixed.transpose(1, 0, 2, 3, 4, 5).reshape(batch_inputs, length, QUERY_HEADS * HEAD_SIZE)

def layer(x, params):
    attn_gain, w_query, key_weight, value_weight, qk_gain, w_out, ffn_gain, w_gate, w_up, w_down = params
    batch_inputs = x.shape[0]
    cosine_table, sine_table = tables(SEQUENCE_TOKENS)
    normalized_input = lower_precision(rms_norm(x, attn_gain))
    q_lin = lower_precision_backward(matrix_product(normalized_input, w_query)).reshape(batch_inputs, SEQUENCE_TOKENS, QUERY_HEADS, HEAD_SIZE)
    key_linear = lower_precision_backward(matrix_product(normalized_input, key_weight)).reshape(batch_inputs, SEQUENCE_TOKENS, KEY_VALUE_HEADS, HEAD_SIZE)
    value_rows = lower_precision(lower_precision_backward(matrix_product(normalized_input, value_weight))).reshape(batch_inputs, SEQUENCE_TOKENS, KEY_VALUE_HEADS, HEAD_SIZE)
    query_rows = lower_precision(rotary_apply(rms_norm(q_lin, qk_gain[:HEAD_SIZE]), cosine_table, sine_table))
    key = lower_precision(rotary_apply(rms_norm(key_linear, qk_gain[HEAD_SIZE:]), cosine_table, sine_table))
    mixed = lower_precision(lower_precision_backward(attend(query_rows, key, value_rows)))
    resid = x + lower_precision_backward(matrix_product(mixed, w_out))
    normed2 = lower_precision(rms_norm(resid, ffn_gain))
    gate = lower_precision_backward(matrix_product(normed2, w_gate))
    upper = lower_precision_backward(matrix_product(normed2, w_up))
    hidden = lower_precision(jax.nn.silu(gate) * upper)
    return resid + matrix_product(hidden, w_down)

def reference(inputs, attn_gain, w_query, key_weight, value_weight, qk_gain, w_out, ffn_gain, w_gate, w_up, w_down, cotangent):
    params = tuple((p.astype(jnp.float32) for p in (attn_gain, w_query, key_weight, value_weight, qk_gain, w_out, ffn_gain, w_gate, w_up, w_down)))
    groups_in = inputs.reshape(N_OUTER, SEQS, SEQUENCE_TOKENS, MODEL_WIDTH)
    groups_cot = cotangent.reshape(N_OUTER, SEQS, SEQUENCE_TOKENS, MODEL_WIDTH)

    def step(totals, pair):
        block_in, block_cot = pair
        output, pull = jax.vjp(layer, block_in.astype(jnp.float32), params)
        d_in, d_params = pull(block_cot.astype(jnp.float32))
        totals = tuple((a + b for a, b in zip(totals, d_params)))
        return (totals, (output.astype(jnp.bfloat16), d_in))
    zeros = tuple((jnp.zeros_like(p) for p in params))
    grads, (outputs, d_ins) = lax.scan(step, zeros, (groups_in, groups_cot))
    return (outputs.reshape(SEQS * N_OUTER, SEQUENCE_TOKENS, MODEL_WIDTH), d_ins.reshape(SEQS * N_OUTER, SEQUENCE_TOKENS, MODEL_WIDTH), grads[0], grads[1], grads[2], grads[3], grads[4], grads[5], grads[6], grads[7], grads[8], grads[9])
```

```python
import jax
import jax.numpy as jnp
from jax import lax
from jax.sharding import Mesh, PartitionSpec as P

QUERY_HEADS = 24
KEY_VALUE_HEADS = 6
HEAD_SIZE = 64
BLOCK = 256
EPS = 1e-06
NEGATIVE = -1e30
ALL = ("inner", "plane", "core")
BF = jnp.bfloat16
F32 = jnp.float32


def mm(left, right):
    return jnp.dot(left, right, preferred_element_type=F32)


def mm_tn(left, right):
    return lax.dot_general(left, right, (((0,), (0,)), ((), ())), preferred_element_type=F32)


def mm_nt(left, right):
    return lax.dot_general(left, right, (((1,), (1,)), ((), ())), preferred_element_type=F32)


def rms_norm(v, gain):
    inverse = lax.rsqrt(jnp.mean(v * v, axis=-1, keepdims=True) + EPS)
    return v * inverse * gain, inverse


def rms_back(v, inverse, gain, grad):
    scaled = grad * gain
    back = inverse * scaled - v * inverse**3 * jnp.mean(scaled * v, axis=-1, keepdims=True)
    return back, grad * v * inverse


def rotary_apply(v, cosine, sine):
    half = HEAD_SIZE // 2
    turned = jnp.concatenate([-v[..., half:], v[..., :half]], axis=-1)
    return v * cosine + turned * sine


def rotary_back(grad, cosine, sine):
    half = HEAD_SIZE // 2
    times = grad * sine
    return grad * cosine + jnp.concatenate([times[..., half:], -times[..., :half]], axis=-1)


def make_body(n_inner, n_plane):
    n_dev = n_inner * n_plane * 2

    def core_swap(v):
        return lax.ppermute(v, "core", [(0, 1), (1, 0)])

    def flip(v, axis, size, bit):
        return lax.ppermute(v, axis, [(i, i ^ bit) for i in range(size)])

    def gather_inner(v, here):
        held = v[None]
        bit = n_inner // 2
        while bit:
            other = flip(held, "inner", n_inner, bit)
            high = (here & bit) != 0
            pair = jnp.stack([jnp.where(high, other, held), jnp.where(high, held, other)], axis=1)
            held = pair.reshape((-1,) + v.shape)
            bit //= 2
        return held

    def scatter_inner(v, here):
        held = v
        bit = 1
        while bit < n_inner:
            pair = held.reshape((held.shape[0] // 2, 2) + v.shape[1:])
            high = ((here & bit) != 0).astype(jnp.int32)
            keep = lax.dynamic_index_in_dim(pair, high, 1, keepdims=False)
            send = lax.dynamic_index_in_dim(pair, 1 - high, 1, keepdims=False)
            other = flip(send, "inner", n_inner, bit)
            held = keep.astype(F32) + other.astype(F32)
            bit *= 2
            if bit < n_inner:
                held = held.astype(BF)
        return held[0].astype(F32)

    def gather_ffn(rows, here):
        held = gather_inner(rows, here)
        whole = lax.all_gather(held, "plane", axis=1, tiled=True)
        return whole.reshape(-1, rows.shape[1])

    def scatter_ffn(whole, here):
        r = whole.shape[0] // (n_inner * n_plane)
        if r % 16:
            held = whole.reshape(n_inner, n_plane, r, whole.shape[1])
            part = lax.psum_scatter(held, "plane", scatter_dimension=1)
        else:
            held = whole.reshape(n_inner, n_plane * r, whole.shape[1])
            part = lax.psum_scatter(held, "plane", scatter_dimension=1, tiled=True)
        return scatter_inner(part, here)

    def butterfly_sum(v):
        for axis, size in (("core", 2), ("plane", n_plane), ("inner", n_inner)):
            bit = 1
            while bit < size:
                v = v + flip(v, axis, size, bit)
                bit *= 2
        return v

    def body(x_in, attn_gain, w_query, w_key, w_value, qk_gain, w_out, ffn_gain, w_gate, w_up, w_down, dy_in):
        here = lax.axis_index("inner")
        core = lax.axis_index("core")
        flat = (here * n_plane + lax.axis_index("plane")) * 2 + core
        seqs, span, width = x_in.shape
        rows = seqs * span
        groups = QUERY_HEADS // KEY_VALUE_HEADS
        scale = HEAD_SIZE ** (-0.5)
        length = span * n_inner
        q_width = w_query.shape[1]
        kv_width = w_key.shape[1]
        per = w_query.shape[0]
        half = w_gate.shape[1] // 2

        extra = jnp.zeros((per, 128), BF)
        extra = extra.at[:, 0].set(attn_gain).at[:, 1].set(ffn_gain)
        extra = extra.at[: qk_gain.shape[0], 2].set(qk_gain)
        packed = jnp.concatenate([w_query, w_key, w_value, extra], axis=1)
        packed = lax.all_gather(packed, ALL, axis=0, tiled=True)
        qkv_width = q_width + 2 * kv_width
        wqkv = packed[:, :qkv_width]
        tail = packed[:, qkv_width : qkv_width + 3].astype(F32)
        g_one = tail[:, 0]
        g_two = tail[:, 1]
        g_qk = tail[:, 2].reshape(n_dev, per)[:, : qk_gain.shape[0]].reshape(-1)
        g_query, g_key = g_qk[:HEAD_SIZE], g_qk[HEAD_SIZE:]
        wo = lax.all_gather(w_out, ALL, axis=0, tiled=True)

        def column_half(w):
            mine = lax.dynamic_slice_in_dim(w, core * half, half, axis=1)
            theirs = lax.dynamic_slice_in_dim(w, (1 - core) * half, half, axis=1)
            got = core_swap(theirs)
            return jnp.where(core == 0, jnp.concatenate([mine, got]), jnp.concatenate([got, mine]))

        spread = [(s, 2 * (s % (n_dev // 2)) + s // (n_dev // 2)) for s in range(n_dev)]
        wg = gather_ffn(column_half(w_gate), here)
        wu = gather_ffn(column_half(w_up), here)
        wd = gather_ffn(lax.ppermute(w_down, ALL, spread), here)

        dy = dy_in.reshape(rows, width)
        dy_both = jnp.concatenate([dy, core_swap(dy)])

        base = here * span
        positions = (base + jnp.arange(span)).astype(F32)
        freq = 10000.0 ** (-jnp.arange(HEAD_SIZE // 2, dtype=F32) * 2.0 / HEAD_SIZE)
        angle = positions[:, None] * freq[None, :]
        cosine = jnp.concatenate([jnp.cos(angle), jnp.cos(angle)], axis=-1)[None, :, None, :]
        sine = jnp.concatenate([jnp.sin(angle), jnp.sin(angle)], axis=-1)[None, :, None, :]
        x = x_in.reshape(rows, width).astype(F32)
        normed, inv_one = rms_norm(x, g_one)
        normed_b = normed.astype(BF)
        lin = mm(normed_b, wqkv)
        q_lin = lin[:, :q_width].reshape(seqs, span, QUERY_HEADS, HEAD_SIZE)
        k_lin = lin[:, q_width : q_width + kv_width].reshape(seqs, span, KEY_VALUE_HEADS, HEAD_SIZE)
        q_normed, inv_query = rms_norm(q_lin, g_query)
        k_normed, inv_key = rms_norm(k_lin, g_key)
        query = rotary_apply(q_normed, cosine, sine).astype(BF)
        key = rotary_apply(k_normed, cosine, sine).astype(BF).reshape(seqs, span, kv_width)
        value = lin[:, q_width + kv_width :].astype(BF).reshape(seqs, span, kv_width)
        kv = jnp.concatenate([key, value], axis=-1)
        row_block = (base + jnp.arange(groups * span) % span) // BLOCK
        allowed = (jnp.arange(length) // BLOCK)[None, :] <= row_block[:, None]

        def by_head(v):
            return v.reshape(span, KEY_VALUE_HEADS, groups, HEAD_SIZE).transpose(1, 2, 0, 3).reshape(
                KEY_VALUE_HEADS, groups * span, HEAD_SIZE
            )

        def by_token(v):
            return v.reshape(KEY_VALUE_HEADS, groups, span, HEAD_SIZE).transpose(2, 0, 1, 3).reshape(
                span, QUERY_HEADS * HEAD_SIZE
            )

        def scores_of(q, k):
            return jnp.where(allowed, mm_nt(q, k) * scale, NEGATIVE)

        def forward_block(triple):
            q, k, v = triple
            scores = scores_of(q, k)
            top = jnp.max(scores, axis=-1, keepdims=True)
            expo = jnp.exp(scores - top)
            total = jnp.sum(expo, axis=-1, keepdims=True)
            return mm((expo / total).astype(BF), v), (top + jnp.log(total))[:, 0]

        kept = []
        mixed = []
        for s in range(seqs):
            both = gather_inner(kv[s], here).reshape(length, 2, KEY_VALUE_HEADS, HEAD_SIZE)
            both = both.transpose(1, 2, 0, 3)
            q_heads = by_head(query[s])
            attended, lse = lax.map(forward_block, (q_heads, both[0], both[1]))
            kept.append((q_heads, both[0], both[1], lse))
            mixed.append(by_token(attended.astype(BF)))
        mixed = jnp.concatenate(mixed)

        resid = x + mm(mixed, wo)
        normed2, inv_two = rms_norm(resid, g_two)
        n2 = normed2.astype(BF)
        n2_both = jnp.concatenate([n2, core_swap(n2)])
        gate = mm(n2_both, wg)
        up = mm(n2_both, wu)
        sigma = jax.nn.sigmoid(gate)
        active = gate * sigma
        hidden = (active * up).astype(BF)
        theirs = core_swap(mm(hidden[rows:], wd).astype(BF))
        output = resid + (mm(hidden[:rows], wd) + theirs.astype(F32))
        result = output.astype(BF).reshape(seqs, span, width)

        grad_down = mm_tn(hidden, dy_both).astype(BF)
        d_down = lax.ppermute(
            scatter_ffn(grad_down, here).astype(BF), ALL, [(b, a) for a, b in spread]
        ).astype(F32)
        d_hidden = mm_nt(dy_both, wd)
        dg = (d_hidden * up * (sigma * (1.0 + gate * (1.0 - sigma)))).astype(BF)
        du = (d_hidden * active).astype(BF)

        def column_whole(part):
            pair = part.astype(BF).reshape(2, per, half)
            mine = lax.dynamic_index_in_dim(pair, core, 0, keepdims=False)
            got = core_swap(lax.dynamic_index_in_dim(pair, 1 - core, 0, keepdims=False))
            return jnp.where(
                core == 0,
                jnp.concatenate([mine, got], axis=1),
                jnp.concatenate([got, mine], axis=1),
            ).astype(F32)

        d_gate = column_whole(scatter_ffn(mm_tn(n2_both, dg).astype(BF), here))
        d_up = column_whole(scatter_ffn(mm_tn(n2_both, du).astype(BF), here))
        theirs = core_swap((mm_nt(dg[rows:], wg) + mm_nt(du[rows:], wu)).astype(BF))
        dn2 = mm_nt(dg[:rows], wg) + mm_nt(du[:rows], wu) + theirs.astype(F32)
        back_two, terms_two = rms_back(resid, inv_two, g_two, dn2)
        grad_gain_two = jnp.sum(terms_two, axis=0)
        d_resid = dy.astype(F32) + back_two

        def scatter_attn(whole):
            r = whole.shape[0] // n_dev
            held = whole.reshape(n_dev // 2, 2, r, -1)
            mine = lax.dynamic_index_in_dim(held, core, 1, keepdims=False)
            got = core_swap(lax.dynamic_index_in_dim(held, 1 - core, 1, keepdims=False))
            held = (mine.astype(F32) + got.astype(F32)).astype(BF)
            return scatter_ffn(held.reshape(whole.shape[0] // 2, -1), here)

        drb = d_resid.astype(BF)
        d_out = scatter_attn(mm_tn(mixed, drb).astype(BF))
        dm = mm_nt(drb, wo).astype(BF).reshape(seqs, span, -1)

        def backward_block(quintet):
            q, k, v, d, lse = quintet
            prob = jnp.exp(scores_of(q, k) - lse[:, None])
            d_prob = mm_nt(d, v)
            ds = (prob * (d_prob - jnp.sum(prob * d_prob, axis=-1, keepdims=True))).astype(BF)
            return mm(ds, k) * scale, mm_tn(ds, q) * scale, mm_tn(prob.astype(BF), d)

        dq = []
        dkv = []
        for s in range(seqs):
            q_heads, k_heads, v_heads, lse = kept[s]
            dq_s, dk_s, dv_s = lax.map(
                backward_block, (q_heads, k_heads, v_heads, by_head(dm[s]), lse)
            )
            dq.append(by_token(dq_s))
            both = jnp.stack([dk_s, dv_s]).astype(BF).transpose(2, 0, 1, 3)
            dkv.append(scatter_inner(both.reshape(n_inner, span, 2 * kv_width), here))
        dq = jnp.stack(dq).reshape(seqs, span, QUERY_HEADS, HEAD_SIZE)
        dkv = jnp.stack(dkv)
        dk = dkv[..., :kv_width].reshape(seqs, span, KEY_VALUE_HEADS, HEAD_SIZE)
        dv = dkv[..., kv_width:].reshape(rows, kv_width)
        back_query, terms_query = rms_back(q_lin, inv_query, g_query, rotary_back(dq, cosine, sine))
        back_key, terms_key = rms_back(k_lin, inv_key, g_key, rotary_back(dk, cosine, sine))
        grad_qk = jnp.concatenate(
            [jnp.sum(terms_query, axis=(0, 1, 2)), jnp.sum(terms_key, axis=(0, 1, 2))]
        )
        d_lin = jnp.concatenate(
            [back_query.reshape(rows, -1), back_key.reshape(rows, -1), dv], axis=1
        ).astype(BF)
        d_qkv = scatter_attn(mm_tn(normed_b, d_lin).astype(BF))
        dn = mm_nt(d_lin, wqkv)
        back_one, terms_one = rms_back(x, inv_one, g_one, dn)
        grad_gain_one = jnp.sum(terms_one, axis=0)
        d_inputs = (d_resid + back_one).reshape(seqs, span, width)

        gains = butterfly_sum(jnp.concatenate([grad_gain_one, grad_gain_two, grad_qk]))
        d_attn_gain = lax.dynamic_slice_in_dim(gains, flat * per, per)
        d_ffn_gain = lax.dynamic_slice_in_dim(gains, width + flat * per, per)
        n_qk = qk_gain.shape[0]
        d_qk = lax.dynamic_slice_in_dim(gains, 2 * width + flat * n_qk, n_qk)
        return (
            result,
            d_inputs,
            d_attn_gain,
            d_qkv[:, :q_width],
            d_qkv[:, q_width : q_width + kv_width],
            d_qkv[:, q_width + kv_width :],
            d_qk,
            d_out,
            d_ffn_gain,
            d_gate,
            d_up,
            d_down,
        )

    return body


def solution(mesh):
    n_inner = mesh.shape["inner"]
    n_plane = mesh.shape["outer"] // 2
    fine = Mesh(mesh.devices.reshape(n_inner, n_plane, 2), ALL)
    tokens = P(("plane", "core"), "inner", None)
    vec = P(ALL)
    mat = P(ALL, None)
    return jax.shard_map(
        make_body(n_inner, n_plane),
        mesh=fine,
        in_specs=(tokens, vec, mat, mat, mat, vec, mat, vec, mat, mat, mat, tokens),
        out_specs=(tokens, tokens, vec, mat, mat, mat, vec, mat, vec, mat, mat, mat),
        check_vma=False,
    )
```

```python
import jax
import jax.numpy as jnp
from jax import lax
from jax.experimental import pallas as pl
from jax.experimental.pallas import tpu as pltpu
from jax.sharding import Mesh, PartitionSpec as P

QUERY_HEADS = 24
KEY_VALUE_HEADS = 6
HEAD_SIZE = 64
BLOCK = 256
EPS = 1e-06
LOG2E = 1.4426950408889634
TP = ("pair", "core")
INNER = ("line", "pair")
ALL = ("line", "pair", "plane", "core")
BF = jnp.bfloat16
F32 = jnp.float32


NT = (((1,), (1,)), ((), ()))
NN = (((1,), (0,)), ((), ()))
TN = (((0,), (0,)), ((), ()))


def dot(a, b, dims):
    return lax.dot_general(a, b, dims, preferred_element_type=F32)


def turn(v):
    half = HEAD_SIZE // 2
    return jnp.concatenate([-v[:, half:], v[:, :half]], axis=1)


def turn_back(v):
    half = HEAD_SIZE // 2
    return jnp.concatenate([v[:, half:], -v[:, :half]], axis=1)


def make_attention(span, length, n_kv, groups, unit):
    pairs = n_kv // 2
    wide = 2 * groups * HEAD_SIZE
    scale = HEAD_SIZE ** (-0.5)
    tall = groups * span

    def queries(q_ref, gain, cosine, sine, g):
        out = []
        for h in range(groups):
            at = (g * groups + h) * HEAD_SIZE
            v = q_ref[:, at : at + HEAD_SIZE]
            inv = lax.rsqrt(jnp.mean(v * v, axis=1, keepdims=True) + EPS)
            n = v * inv * gain
            out.append(((n * cosine + turn(n) * sine) * (scale * LOG2E)).astype(BF))
        return jnp.concatenate(out, axis=0)

    def forward_kernel(seen_ref, q_ref, k_ref, v_ref, gain_ref, cos_ref, sin_ref, o_ref, l_ref):
        gain = gain_ref[...]
        cosine = cos_ref[...]
        sine = sin_ref[...]
        ones = jnp.ones((unit, HEAD_SIZE), BF)
        q_all = [queries(q_ref, gain, cosine, sine, g) for g in range(2)]

        def step(i, accs):
            at = pl.ds(pl.multiple_of(i * unit, unit), unit)
            out = []
            for g in range(2):
                lanes = slice(g * HEAD_SIZE, (g + 1) * HEAD_SIZE)
                k = k_ref[at, :][:, lanes]
                v = jnp.concatenate([v_ref[at, :][:, lanes], ones], axis=1)
                e = jnp.exp2(dot(q_all[g], k, NT)).astype(BF)
                out.append(accs[g] + dot(e, v, NN))
            return tuple(out)

        zero = jnp.zeros((tall, 2 * HEAD_SIZE), F32)
        accs = lax.fori_loop(0, seen_ref[0], step, (zero, zero))
        for g in range(2):
            inv = 1.0 / accs[g][:, HEAD_SIZE:]
            o = (accs[g][:, :HEAD_SIZE] * inv).astype(BF)
            for h in range(groups):
                at = (g * groups + h) * HEAD_SIZE
                o_ref[:, at : at + HEAD_SIZE] = o[h * span : (h + 1) * span]
                l_ref[:, at : at + HEAD_SIZE] = inv[h * span : (h + 1) * span]

    def backward_kernel(
        seen_ref, q_ref, k_ref, v_ref, gain_ref, cos_ref, sin_ref, o_ref, l_ref, d_ref,
        dq_ref, dk_ref, dv_ref, dg_ref, acc_ref,
    ):
        gain = gain_ref[...]
        cosine = cos_ref[...]
        sine = sin_ref[...]
        ones = jnp.ones((unit, HEAD_SIZE), BF)
        q_all = []
        d_all = []
        d_aug = []
        for g in range(2):
            q_all.append(queries(q_ref, gain, cosine, sine, g))
            rows = []
            more = []
            for h in range(groups):
                at = (g * groups + h) * HEAD_SIZE
                d = d_ref[:, at : at + HEAD_SIZE].astype(F32)
                inv = l_ref[:, at : at + HEAD_SIZE]
                o = o_ref[:, at : at + HEAD_SIZE].astype(F32)
                delta = -jnp.sum(d * o, axis=1, keepdims=True) * inv
                top = delta.astype(BF)
                low = (delta - top.astype(F32)).astype(BF)
                lane = lax.broadcasted_iota(jnp.int32, (span, HEAD_SIZE), 1)
                side = jnp.where(lane == 0, top.astype(F32), jnp.where(lane == 1, low.astype(F32), 0.0))
                rows.append((d * inv).astype(BF))
                more.append(side.astype(BF))
            d_all.append(jnp.concatenate(rows, axis=0))
            d_aug.append(jnp.concatenate([d_all[g], jnp.concatenate(more, axis=0)], axis=1))
        acc_ref[...] = jnp.zeros_like(acc_ref)
        dk_ref[...] = jnp.zeros_like(dk_ref)
        dv_ref[...] = jnp.zeros_like(dv_ref)

        def step(i, carry):
            at = pl.ds(pl.multiple_of(i * unit, unit), unit)
            dk = []
            dv = []
            for g in range(2):
                lanes = slice(g * HEAD_SIZE, (g + 1) * HEAD_SIZE)
                k = k_ref[at, :][:, lanes]
                v = jnp.concatenate([v_ref[at, :][:, lanes], ones], axis=1)
                e = jnp.exp2(dot(k, q_all[g], NT))
                ds = (e * dot(v, d_aug[g], NT)).astype(BF)
                dv.append(dot(e.astype(BF), d_all[g], NN))
                dk.append(dot(ds, q_all[g], NN))
                acc_ref[g] += dot(ds, k, TN)
            dk_ref[at, :] = (jnp.concatenate(dk, axis=1) * (1.0 / LOG2E)).astype(BF)
            dv_ref[at, :] = jnp.concatenate(dv, axis=1).astype(BF)
            return carry

        lax.fori_loop(0, seen_ref[0], step, 0)
        total = jnp.zeros((span, HEAD_SIZE), F32)
        for g in range(2):
            for h in range(groups):
                at = (g * groups + h) * HEAD_SIZE
                dr = acc_ref[g, h * span : (h + 1) * span, :] * scale
                v = q_ref[:, at : at + HEAD_SIZE]
                inv = lax.rsqrt(jnp.mean(v * v, axis=1, keepdims=True) + EPS)
                e = dr * cosine + turn_back(dr * sine)
                scaled = e * gain
                back = inv * scaled - v * inv**3 * jnp.mean(scaled * v, axis=1, keepdims=True)
                total = total + e * v * inv
                dq_ref[:, at : at + HEAD_SIZE] = back.astype(BF)
        dg_ref[0] = jnp.broadcast_to(jnp.sum(total, axis=0, keepdims=True), (8, HEAD_SIZE))

    def window(at):
        return pl.BlockSpec((span, wide), lambda j, s: (at, j))

    q_spec = window(0)
    k_spec = pl.BlockSpec((length, 2 * HEAD_SIZE), lambda j, s: (0, j))
    v_spec = pl.BlockSpec((length, 2 * HEAD_SIZE), lambda j, s: (0, pairs + j))
    row = pl.BlockSpec((1, HEAD_SIZE), lambda j, s: (0, 0))
    table = pl.BlockSpec((span, HEAD_SIZE), lambda j, s: (0, 0))
    q_width = pairs * wide
    kv_width = n_kv * HEAD_SIZE
    params = pltpu.CompilerParams(dimension_semantics=("arbitrary",))
    flops = 4 * n_kv * tall * length * HEAD_SIZE

    def forward(at, seen, q_lin, kv, gain, cosine, sine):
        return pl.pallas_call(
            forward_kernel,
            grid_spec=pltpu.PrefetchScalarGridSpec(
                num_scalar_prefetch=1,
                grid=(pairs,),
                in_specs=[window(at), k_spec, v_spec, row, table, table],
                out_specs=[q_spec, q_spec],
            ),
            out_shape=[
                jax.ShapeDtypeStruct((span, q_width), BF),
                jax.ShapeDtypeStruct((span, q_width), F32),
            ],
            compiler_params=params,
            cost_estimate=pl.CostEstimate(
                flops=flops * 4, transcendentals=n_kv * tall * length, bytes_accessed=8 * span * q_width
            ),
            name="attention_forward",
        )(seen, q_lin, kv, kv, gain, cosine, sine)

    def backward(at, seen, q_lin, kv, gain, cosine, sine, o, inv, d):
        return pl.pallas_call(
            backward_kernel,
            grid_spec=pltpu.PrefetchScalarGridSpec(
                num_scalar_prefetch=1,
                grid=(pairs,),
                in_specs=[window(at), k_spec, v_spec, row, table, table, q_spec, q_spec, window(at)],
                out_specs=[
                    q_spec,
                    k_spec,
                    k_spec,
                    pl.BlockSpec((1, 8, HEAD_SIZE), lambda j, s: (j, 0, 0)),
                ],
                scratch_shapes=[pltpu.VMEM((2, tall, HEAD_SIZE), F32)],
            ),
            out_shape=[
                jax.ShapeDtypeStruct((span, q_width), BF),
                jax.ShapeDtypeStruct((length, kv_width), BF),
                jax.ShapeDtypeStruct((length, kv_width), BF),
                jax.ShapeDtypeStruct((pairs, 8, HEAD_SIZE), F32),
            ],
            compiler_params=params,
            cost_estimate=pl.CostEstimate(
                flops=flops * 10, transcendentals=n_kv * tall * length, bytes_accessed=16 * span * q_width
            ),
            name="attention_backward",
        )(seen, q_lin, kv, kv, gain, cosine, sine, o, inv, d)

    return forward, backward


def make_keys(seqs, span, n_kv):
    kv_width = n_kv * HEAD_SIZE

    def forward_kernel(v_ref, gain_ref, cos_ref, sin_ref, o_ref):
        gain = gain_ref[...]
        cosine = cos_ref[...]
        sine = sin_ref[...]
        out = []
        for g in range(n_kv):
            v = v_ref[:, g * HEAD_SIZE : (g + 1) * HEAD_SIZE]
            n = v * lax.rsqrt(jnp.mean(v * v, axis=1, keepdims=True) + EPS) * gain
            out.append(n * cosine + turn(n) * sine)
        o_ref[:, :kv_width] = jnp.concatenate(out, axis=1).astype(BF)
        o_ref[:, kv_width:] = v_ref[:, kv_width:].astype(BF)

    def backward_kernel(v_ref, d_ref, gain_ref, cos_ref, sin_ref, o_ref, dg_ref):
        gain = gain_ref[...]
        cosine = cos_ref[...]
        sine = sin_ref[...]
        out = []
        total = jnp.zeros((span, HEAD_SIZE), F32)
        for g in range(n_kv):
            v = v_ref[:, g * HEAD_SIZE : (g + 1) * HEAD_SIZE]
            d = d_ref[:, g * HEAD_SIZE : (g + 1) * HEAD_SIZE]
            inv = lax.rsqrt(jnp.mean(v * v, axis=1, keepdims=True) + EPS)
            e = d * cosine + turn_back(d * sine)
            scaled = e * gain
            out.append(inv * scaled - v * inv**3 * jnp.mean(scaled * v, axis=1, keepdims=True))
            total = total + e * v * inv
        o_ref[:, :kv_width] = jnp.concatenate(out, axis=1).astype(BF)
        o_ref[:, kv_width:] = d_ref[:, kv_width:].astype(BF)
        dg_ref[...] = jnp.broadcast_to(jnp.sum(total, axis=0, keepdims=True), (8, HEAD_SIZE))

    row = pl.BlockSpec((1, HEAD_SIZE), lambda i: (0, 0))
    table = pl.BlockSpec((span, HEAD_SIZE), lambda i: (0, 0))
    params = pltpu.CompilerParams(dimension_semantics=("arbitrary",))

    def window(at):
        return pl.BlockSpec((span, 2 * kv_width), lambda i: (at, 0))

    cost = pl.CostEstimate(
        flops=20 * span * kv_width, transcendentals=span * n_kv, bytes_accessed=16 * span * kv_width
    )

    def forward(at, lin, gain, cosine, sine):
        return pl.pallas_call(
            forward_kernel,
            grid=(1,),
            in_specs=[window(at), row, table, table],
            out_specs=window(0),
            out_shape=jax.ShapeDtypeStruct((span, 2 * kv_width), BF),
            compiler_params=params,
            cost_estimate=cost,
            name="key_forward",
        )(lin, gain, cosine, sine)

    def backward(at, lin, d, gain, cosine, sine):
        return pl.pallas_call(
            backward_kernel,
            grid=(1,),
            in_specs=[window(at), window(0), row, table, table],
            out_specs=[window(0), pl.BlockSpec((8, HEAD_SIZE), lambda i: (0, 0))],
            out_shape=[
                jax.ShapeDtypeStruct((span, 2 * kv_width), BF),
                jax.ShapeDtypeStruct((8, HEAD_SIZE), F32),
            ],
            compiler_params=params,
            cost_estimate=cost,
            name="key_backward",
        )(lin, d, gain, cosine, sine)

    return forward, backward


def mm(left, right):
    return dot(left, right, NN)


def mm_tn(left, right):
    return dot(left, right, TN)


def mm_nt(left, right):
    return dot(left, right, NT)


def rms_norm(v, gain):
    inverse = lax.rsqrt(jnp.mean(v * v, axis=-1, keepdims=True) + EPS)
    return v * inverse * gain, inverse


def rms_back(v, inverse, gain, grad):
    scaled = grad * gain
    back = inverse * scaled - v * inverse**3 * jnp.mean(scaled * v, axis=-1, keepdims=True)
    return back, grad * v * inverse


def tie(*values):
    return lax.optimization_barrier(values)


def make_body(n_line, n_plane):
    n_inner = n_line * 2
    n_tp = 4
    n_group = n_line * n_plane
    n_dev = n_group * n_tp

    def flip(v, axis, size, bit):
        return lax.ppermute(v, axis, [(i, i ^ bit) for i in range(size)])

    def core_swap(v):
        return flip(v, "core", 2, 1)

    def pair_swap(v):
        return flip(v, "pair", 2, 1)

    def by_source(pieces, here):
        held = jnp.stack(pieces)
        shape = held.shape
        bit = 1
        while bit < len(pieces):
            split = held.reshape((-1, 2, bit) + shape[1:])
            turned = jnp.concatenate([split[:, 1:], split[:, :1]], axis=1)
            held = jnp.where((here & bit) != 0, turned, split).reshape(shape)
            bit *= 2
        return held

    def exchange(piece_of, axes, size, here):
        pieces = [piece_of(here)]
        pieces += [flip(piece_of(here ^ b), axes, size, b) for b in range(1, size)]
        return pieces

    def gather_inner(v, here):
        held = v[None]
        bit = n_inner // 2
        while bit:
            other = flip(held, INNER, n_inner, bit)
            high = (here & bit) != 0
            pair = jnp.stack([jnp.where(high, other, held), jnp.where(high, held, other)], axis=1)
            held = pair.reshape((-1,) + v.shape)
            bit //= 2
        return held

    def scatter_inner(v, here):
        held = v
        bit = 1
        while bit < n_inner:
            pair = held.reshape((held.shape[0] // 2, 2) + v.shape[1:])
            high = ((here & bit) != 0).astype(jnp.int32)
            keep = lax.dynamic_index_in_dim(pair, high, 1, keepdims=False)
            send = lax.dynamic_index_in_dim(pair, 1 - high, 1, keepdims=False)
            other = flip(send, INNER, n_inner, bit)
            held = keep.astype(F32) + other.astype(F32)
            bit *= 2
            if bit < n_inner:
                held = held.astype(BF)
        return held[0].astype(F32)

    def sum_pieces(part, axes, size, here):
        pieces = exchange(
            lambda k: lax.dynamic_index_in_dim(part, k, 0, keepdims=False), axes, size, here
        )
        total = pieces[0].astype(F32)
        for piece in pieces[1:]:
            total = total + piece.astype(F32)
        return total

    def spread_line(rows, line):
        return by_source(exchange(lambda k: rows, "line", n_line, line), line)

    def whole_rows(held, width):
        return lax.all_gather(held, "plane", axis=1, tiled=True).reshape(-1, width)

    def scatter_plane(whole, lead):
        r = whole.shape[0] // (lead * n_plane)
        if r % 16:
            held = whole.reshape(lead, n_plane, r, whole.shape[1])
            return lax.psum_scatter(held, "plane", scatter_dimension=1)
        held = whole.reshape(lead, n_plane * r, whole.shape[1])
        return lax.psum_scatter(held, "plane", scatter_dimension=1, tiled=True)

    def butterfly_sum(v):
        for axis, size in (("core", 2), ("pair", 2), ("plane", n_plane), ("line", n_line)):
            bit = 1
            while bit < size:
                v = v + flip(v, axis, size, bit)
                bit *= 2
        return v

    def near_and_far(chunks):
        far = jnp.concatenate([pair_swap(v) for v in chunks])
        near = jnp.concatenate(chunks)
        return jnp.concatenate([near, core_swap(near)]), jnp.concatenate([far, core_swap(far)])

    def fold(partial):
        half = partial.shape[0] // 2
        return partial[:half] + core_swap(partial[half:].astype(BF)).astype(F32)

    def body(x_in, attn_gain, w_query, w_key, w_value, qk_gain, w_out, ffn_gain, w_gate, w_up, w_down, dy_in):
        line = lax.axis_index("line")
        core = lax.axis_index("core")
        here = line * 2 + lax.axis_index("pair")
        tp = lax.axis_index("pair") * 2 + core
        flat = (here * n_plane + lax.axis_index("plane")) * 2 + core
        seqs, span, width = x_in.shape
        rows = seqs * span
        groups = QUERY_HEADS // KEY_VALUE_HEADS
        length = span * n_inner
        q_width = w_query.shape[1]
        kv_width = w_key.shape[1]
        per = w_query.shape[0]
        part = w_gate.shape[1] // n_tp

        def column_part(w):
            pieces = exchange(
                lambda k: lax.dynamic_slice_in_dim(w, k * part, part, axis=1), TP, n_tp, tp
            )
            return by_source(pieces, tp).reshape(2, 2 * per, part)

        def holder(s):
            quarter, group = divmod(s, n_group)
            at_line, at_plane = divmod(group, n_plane)
            return ((at_line * 2 + quarter // 2) * n_plane + at_plane) * 2 + quarter % 2

        spread = [(s, holder(s)) for s in range(n_dev)]
        extra = jnp.zeros((per, 128), BF)
        extra = extra.at[:, 0].set(attn_gain).at[:, 1].set(ffn_gain)
        extra = extra.at[: qk_gain.shape[0], 2].set(qk_gain)
        at_gain = 2 * kv_width
        at_query = at_gain + 128
        at_out = at_query + q_width
        out_rows = jnp.pad(w_out, ((0, per - w_out.shape[0]), (0, 0)))
        packed = jnp.concatenate([w_key, w_value, extra, w_query, out_rows], axis=1)
        packed = lax.all_gather(packed, ALL, axis=0, tiled=True)
        wkv = packed[:, :at_gain]
        wq = packed[:, at_query:at_out]
        wo = packed[:, at_out:].reshape(n_dev, per, width)[:, : w_out.shape[0]].reshape(-1, width)
        tail = packed[:, at_gain : at_gain + 3].astype(F32)
        g_one = tail[:, 0]
        g_two = tail[:, 1]
        g_qk = tail[:, 2].reshape(n_dev, per)[:, : qk_gain.shape[0]].reshape(-1)
        g_query, g_key = g_qk[:HEAD_SIZE], g_qk[HEAD_SIZE:]

        wg = whole_rows(spread_line(column_part(w_gate), line).reshape(n_inner, 2 * per, part), part)
        wu = whole_rows(spread_line(column_part(w_up), line).reshape(n_inner, 2 * per, part), part)
        cut_down = lax.ppermute(w_down, ALL, spread)
        dy = dy_in.reshape(rows, width)

        base = here * span
        positions = (base + jnp.arange(span)).astype(F32)
        freq = 10000.0 ** (-jnp.arange(HEAD_SIZE // 2, dtype=F32) * 2.0 / HEAD_SIZE)
        angle = positions[:, None] * freq[None, :]
        cosine = jnp.concatenate([jnp.cos(angle), jnp.cos(angle)], axis=-1)
        sine = jnp.concatenate([jnp.sin(angle), jnp.sin(angle)], axis=-1)
        unit = min(BLOCK, length)
        seen = ((base // BLOCK + 1) * (BLOCK // unit)).astype(jnp.int32).reshape(1)
        attend, attend_back = make_attention(span, length, KEY_VALUE_HEADS, groups, unit)
        gain_row = g_query.reshape(1, HEAD_SIZE)

        x = x_in.reshape(rows, width).astype(F32)
        normed, inv_one = rms_norm(x, g_one)
        normed_b = normed.astype(BF)
        kv_lin = mm(normed_b, wkv)
        gain_key = g_key.reshape(1, HEAD_SIZE)
        make_key, make_key_back = make_keys(seqs, span, KEY_VALUE_HEADS)
        kv = [make_key(s, kv_lin, gain_key, cosine, sine) for s in range(seqs)]
        gathered = [gather_inner(v, here).reshape(length, 2 * kv_width) for v in kv]
        q_lin = mm(normed_b, wq)
        gathered[-1], cut_down, dy_in = tie(gathered[-1], cut_down, dy_in)
        dy_near, dy_far = near_and_far(list(dy_in))
        cut_down = spread_line(cut_down, line)
        kept = []
        resids = []
        invs = []
        n2s = []
        for s in range(seqs):
            o, total = attend(s, seen, q_lin, gathered[s], gain_row, cosine, sine)
            if s == seqs - 1:
                o, cut_down = tie(o, cut_down)
                wd = whole_rows(cut_down, width)
            kept.append((o, total))
            resid = x[s * span : (s + 1) * span] + mm(o, wo)
            normed2, inv_two = rms_norm(resid, g_two)
            resids.append(resid)
            invs.append(inv_two)
            n2s.append(normed2.astype(BF))
        mixed = jnp.concatenate([o for o, _ in kept])
        resid = jnp.concatenate(resids)
        inv_two = jnp.concatenate(invs)
        n2_near, n2_far = near_and_far(n2s)

        def expand(n2):
            gate = mm(n2, wg)
            up = mm(n2, wu)
            return gate, up, (gate * jax.nn.sigmoid(gate) * up).astype(BF)

        def expand_back(dy, gate, up):
            d_hidden = mm_nt(dy, wd)
            sigma = jax.nn.sigmoid(gate)
            dg = (d_hidden * up * (sigma * (1.0 + gate * (1.0 - sigma)))).astype(BF)
            return dg, (d_hidden * (gate * sigma)).astype(BF)

        gate_near, up_near, hidden_near = expand(n2_near)
        gate_far, up_far, hidden_far = expand(n2_far)
        hidden = jnp.concatenate([hidden_near, hidden_far])
        n2_all = jnp.concatenate([n2_near, n2_far])

        grad_down = mm_tn(hidden, jnp.concatenate([dy_near, dy_far])).astype(BF)
        wd, grad_down = tie(wd, grad_down)
        down_part = scatter_plane(grad_down, n_line)
        dg_far, du_far = expand_back(dy_far, gate_far, up_far)
        sent = fold(mm_nt(dg_far, wg) + mm_nt(du_far, wu)).astype(BF)
        sent, dy_near = tie(sent, dy_near)
        dg_near, du_near = expand_back(dy_near, gate_near, up_near)
        dn2 = fold(mm_nt(dg_near, wg) + mm_nt(du_near, wu))
        grad_gate = mm_tn(n2_all, jnp.concatenate([dg_near, dg_far])).astype(BF)
        grad_up = mm_tn(n2_all, jnp.concatenate([du_near, du_far])).astype(BF)
        got = pair_swap(sent)
        gate_part = scatter_plane(grad_gate, n_inner)
        up_part = scatter_plane(grad_up, n_inner)
        got, dn2, grad_gate, grad_up, down_part = tie(got, dn2, grad_gate, grad_up, down_part)
        down_sum = sum_pieces(down_part, "line", n_line, line).astype(BF)
        dn2 = dn2 + got.astype(F32)
        back_two, terms_two = rms_back(resid, inv_two, g_two, dn2)
        grad_gain_two = jnp.sum(terms_two, axis=0)
        d_resid = dy.astype(F32) + back_two

        def column_whole(piece):
            held = piece.astype(BF)
            pieces = exchange(
                lambda k: lax.dynamic_index_in_dim(held, k, 0, keepdims=False), TP, n_tp, tp
            )
            return by_source(pieces, tp).transpose(1, 0, 2).reshape(per, -1).astype(F32)

        def fold_core(whole):
            r = whole.shape[0] // n_dev
            held = whole.reshape(n_dev // 2, 2, r, -1)
            mine = lax.dynamic_index_in_dim(held, core, 1, keepdims=False)
            got = core_swap(lax.dynamic_index_in_dim(held, 1 - core, 1, keepdims=False))
            held = (mine.astype(F32) + got.astype(F32)).astype(BF)
            return held.reshape(whole.shape[0] // 2, -1)

        drb = d_resid.astype(BF)
        dm = mm_nt(drb, wo).astype(BF)
        out_part = scatter_plane(fold_core(mm_tn(mixed, drb).astype(BF)), n_inner)
        dm, down_sum, gate_part = tie(dm, down_sum, gate_part)
        gate_sum = sum_pieces(gate_part.reshape(n_line, n_tp, per, part), "line", n_line, line)
        dq = []
        dkv = []
        gains_q = []
        for s in range(seqs):
            dq_s, dk_s, dv_s, dg_s = attend_back(
                s, seen, q_lin, gathered[s], gain_row, cosine, sine, *kept[s], dm
            )
            dq.append(dq_s)
            gains_q.append(jnp.sum(dg_s[:, 0], axis=0))
            both = jnp.concatenate([dk_s, dv_s], axis=1)
            if s == seqs - 1:
                both, hidden_near, hidden_far, gate_sum = tie(both, hidden_near, hidden_far, gate_sum)
            dkv.append(scatter_inner(both.reshape(n_inner, span, 2 * kv_width), here))
        d_down = lax.ppermute(down_sum, ALL, [(b, a) for a, b in spread]).astype(F32)
        sent = fold(mm(hidden_far, wd)).astype(BF)
        output = resid + (fold(mm(hidden_near, wd)) + pair_swap(sent).astype(F32))
        result = output.astype(BF).reshape(seqs, span, width)
        dkv[-1], up_part, out_part = tie(dkv[-1], up_part, out_part)
        up_sum = sum_pieces(up_part.reshape(n_line, n_tp, per, part), "line", n_line, line)
        d_out = sum_pieces(out_part, INNER, n_inner, here)
        d_kvs = []
        gains_k = []
        for s in range(seqs):
            d_kv_s, dg_s = make_key_back(s, kv_lin, dkv[s], gain_key, cosine, sine)
            d_kvs.append(d_kv_s)
            gains_k.append(dg_s[0])
        grad_qk = jnp.concatenate([sum(gains_q), sum(gains_k)])
        d_lin = jnp.concatenate([jnp.concatenate(dq), jnp.concatenate(d_kvs)], axis=1)
        grad_qkv = mm_tn(normed_b, d_lin).astype(BF)
        qkv_part = scatter_plane(fold_core(grad_qkv), n_inner)
        d_lin, grad_qkv, up_sum, d_out = tie(d_lin, grad_qkv, up_sum, d_out)
        d_gate = column_whole(gate_sum)
        d_up = column_whole(up_sum)
        dn = mm_nt(d_lin[:, :q_width], wq) + mm_nt(d_lin[:, q_width:], wkv)
        back_one, terms_one = rms_back(x, inv_one, g_one, dn)
        grad_gain_one = jnp.sum(terms_one, axis=0)
        d_inputs = (d_resid + back_one).reshape(seqs, span, width)

        gains = butterfly_sum(jnp.concatenate([grad_gain_one, grad_gain_two, grad_qk]))
        qkv_part, d_gate, d_up, d_out, result = tie(qkv_part, d_gate, d_up, d_out, result)
        d_qkv = sum_pieces(qkv_part, INNER, n_inner, here)
        d_attn_gain = lax.dynamic_slice_in_dim(gains, flat * per, per)
        d_ffn_gain = lax.dynamic_slice_in_dim(gains, width + flat * per, per)
        n_qk = qk_gain.shape[0]
        d_qk = lax.dynamic_slice_in_dim(gains, 2 * width + flat * n_qk, n_qk)
        return (
            result,
            d_inputs,
            d_attn_gain,
            d_qkv[:, :q_width],
            d_qkv[:, q_width : q_width + kv_width],
            d_qkv[:, q_width + kv_width :],
            d_qk,
            d_out,
            d_ffn_gain,
            d_gate,
            d_up,
            d_down,
        )

    return body


def solution(mesh):
    n_line = mesh.shape["inner"] // 2
    n_plane = mesh.shape["outer"] // 2
    fine = Mesh(mesh.devices.reshape(n_line, 2, n_plane, 2), ALL)
    tokens = P(("plane", "core"), INNER, None)
    vec = P(ALL)
    mat = P(ALL, None)
    return jax.shard_map(
        make_body(n_line, n_plane),
        mesh=fine,
        in_specs=(tokens, vec, mat, mat, mat, vec, mat, vec, mat, mat, mat, tokens),
        out_specs=(tokens, tokens, vec, mat, mat, mat, vec, mat, vec, mat, mat, mat),
        check_vma=False,
    )
```

```python
import jax
import jax.numpy as jnp
from jax import lax
from jax.experimental import pallas as pl
from jax.experimental.pallas import tpu as pltpu
from jax.sharding import Mesh, PartitionSpec as P

QUERY_HEADS = 24
KEY_VALUE_HEADS = 6
HEAD_SIZE = 64
BLOCK = 256
EPS = 1e-06
LOG2E = 1.4426950408889634
TP = ("pair", "core")
INNER = ("line", "pair")
ALL = ("line", "pair", "plane", "core")
BF = jnp.bfloat16
F32 = jnp.float32
SMALL = pl.CostEstimate(flops=1000, transcendentals=0, bytes_accessed=1000)


NT = (((1,), (1,)), ((), ()))
NN = (((1,), (0,)), ((), ()))
TN = (((0,), (0,)), ((), ()))


def dot(a, b, dims):
    return lax.dot_general(a, b, dims, preferred_element_type=F32)


def turn(v):
    half = HEAD_SIZE // 2
    return jnp.concatenate([-v[:, half:], v[:, :half]], axis=1)


def turn_back(v):
    half = HEAD_SIZE // 2
    return jnp.concatenate([v[:, half:], -v[:, :half]], axis=1)


def make_attention(span, length, n_kv, groups, unit):
    pairs = n_kv // 2
    wide = 2 * groups * HEAD_SIZE
    scale = HEAD_SIZE ** (-0.5)
    tall = groups * span

    def queries(q_ref, gain, cosine, sine, g):
        out = []
        for h in range(groups):
            at = (g * groups + h) * HEAD_SIZE
            v = q_ref[:, at : at + HEAD_SIZE]
            inv = lax.rsqrt(jnp.mean(v * v, axis=1, keepdims=True) + EPS)
            n = v * inv * gain
            out.append(((n * cosine + turn(n) * sine) * (scale * LOG2E)).astype(BF))
        return jnp.concatenate(out, axis=0)

    def forward_kernel(seen_ref, q_ref, k_ref, v_ref, gain_ref, cos_ref, sin_ref, o_ref, l_ref):
        gain = gain_ref[...]
        cosine = cos_ref[...]
        sine = sin_ref[...]
        ones = jnp.ones((unit, HEAD_SIZE), BF)
        q_all = [queries(q_ref, gain, cosine, sine, g) for g in range(2)]

        def step(i, accs):
            at = pl.ds(pl.multiple_of(i * unit, unit), unit)
            out = []
            for g in range(2):
                lanes = slice(g * HEAD_SIZE, (g + 1) * HEAD_SIZE)
                k = k_ref[at, :][:, lanes]
                v = jnp.concatenate([v_ref[at, :][:, lanes], ones], axis=1)
                e = jnp.exp2(dot(q_all[g], k, NT)).astype(BF)
                out.append(accs[g] + dot(e, v, NN))
            return tuple(out)

        zero = jnp.zeros((tall, 2 * HEAD_SIZE), F32)
        accs = lax.fori_loop(0, seen_ref[0], step, (zero, zero))
        for g in range(2):
            inv = 1.0 / accs[g][:, HEAD_SIZE:]
            o = (accs[g][:, :HEAD_SIZE] * inv).astype(BF)
            for h in range(groups):
                at = (g * groups + h) * HEAD_SIZE
                o_ref[:, at : at + HEAD_SIZE] = o[h * span : (h + 1) * span]
                l_ref[:, at : at + HEAD_SIZE] = inv[h * span : (h + 1) * span]

    def backward_kernel(
        seen_ref, q_ref, k_ref, v_ref, gain_ref, cos_ref, sin_ref, o_ref, l_ref, d_ref,
        dq_ref, dk_ref, dv_ref, dg_ref, acc_ref,
    ):
        gain = gain_ref[...]
        cosine = cos_ref[...]
        sine = sin_ref[...]
        ones = jnp.ones((unit, HEAD_SIZE), BF)
        q_all = []
        d_all = []
        d_aug = []
        for g in range(2):
            q_all.append(queries(q_ref, gain, cosine, sine, g))
            rows = []
            more = []
            for h in range(groups):
                at = (g * groups + h) * HEAD_SIZE
                d = d_ref[:, at : at + HEAD_SIZE].astype(F32)
                inv = l_ref[:, at : at + HEAD_SIZE]
                o = o_ref[:, at : at + HEAD_SIZE].astype(F32)
                delta = -jnp.sum(d * o, axis=1, keepdims=True) * inv
                top = delta.astype(BF)
                low = (delta - top.astype(F32)).astype(BF)
                lane = lax.broadcasted_iota(jnp.int32, (span, HEAD_SIZE), 1)
                side = jnp.where(lane == 0, top.astype(F32), jnp.where(lane == 1, low.astype(F32), 0.0))
                rows.append((d * inv).astype(BF))
                more.append(side.astype(BF))
            d_all.append(jnp.concatenate(rows, axis=0))
            d_aug.append(jnp.concatenate([d_all[g], jnp.concatenate(more, axis=0)], axis=1))
        acc_ref[...] = jnp.zeros_like(acc_ref)
        dk_ref[...] = jnp.zeros_like(dk_ref)
        dv_ref[...] = jnp.zeros_like(dv_ref)

        def step(i, carry):
            at = pl.ds(pl.multiple_of(i * unit, unit), unit)
            dk = []
            dv = []
            for g in range(2):
                lanes = slice(g * HEAD_SIZE, (g + 1) * HEAD_SIZE)
                k = k_ref[at, :][:, lanes]
                v = jnp.concatenate([v_ref[at, :][:, lanes], ones], axis=1)
                e = jnp.exp2(dot(k, q_all[g], NT))
                ds = (e * dot(v, d_aug[g], NT)).astype(BF)
                dv.append(dot(e.astype(BF), d_all[g], NN))
                dk.append(dot(ds, q_all[g], NN))
                acc_ref[g] += dot(ds, k, TN)
            dk_ref[at, :] = (jnp.concatenate(dk, axis=1) * (1.0 / LOG2E)).astype(BF)
            dv_ref[at, :] = jnp.concatenate(dv, axis=1).astype(BF)
            return carry

        lax.fori_loop(0, seen_ref[0], step, 0)
        total = jnp.zeros((span, HEAD_SIZE), F32)
        for g in range(2):
            for h in range(groups):
                at = (g * groups + h) * HEAD_SIZE
                dr = acc_ref[g, h * span : (h + 1) * span, :] * scale
                v = q_ref[:, at : at + HEAD_SIZE]
                inv = lax.rsqrt(jnp.mean(v * v, axis=1, keepdims=True) + EPS)
                e = dr * cosine + turn_back(dr * sine)
                scaled = e * gain
                back = inv * scaled - v * inv**3 * jnp.mean(scaled * v, axis=1, keepdims=True)
                total = total + e * v * inv
                dq_ref[:, at : at + HEAD_SIZE] = back.astype(BF)
        dg_ref[0] = jnp.broadcast_to(jnp.sum(total, axis=0, keepdims=True), (8, HEAD_SIZE))

    def window(at):
        return pl.BlockSpec((span, wide), lambda j, s: (at, j))

    q_spec = window(0)
    k_spec = pl.BlockSpec((length, 2 * HEAD_SIZE), lambda j, s: (0, j))
    v_spec = pl.BlockSpec((length, 2 * HEAD_SIZE), lambda j, s: (0, pairs + j))
    row = pl.BlockSpec((1, HEAD_SIZE), lambda j, s: (0, 0))
    table = pl.BlockSpec((span, HEAD_SIZE), lambda j, s: (0, 0))
    q_width = pairs * wide
    kv_width = n_kv * HEAD_SIZE
    params = pltpu.CompilerParams(dimension_semantics=("arbitrary",))

    def forward(at, seen, q_lin, kv, gain, cosine, sine):
        return pl.pallas_call(
            forward_kernel,
            grid_spec=pltpu.PrefetchScalarGridSpec(
                num_scalar_prefetch=1,
                grid=(pairs,),
                in_specs=[window(at), k_spec, v_spec, row, table, table],
                out_specs=[q_spec, q_spec],
            ),
            out_shape=[
                jax.ShapeDtypeStruct((span, q_width), BF),
                jax.ShapeDtypeStruct((span, q_width), F32),
            ],
            compiler_params=params,
            cost_estimate=SMALL,
            name="attention_forward",
        )(seen, q_lin, kv, kv, gain, cosine, sine)

    def backward(at, seen, q_lin, kv, gain, cosine, sine, o, inv, d):
        return pl.pallas_call(
            backward_kernel,
            grid_spec=pltpu.PrefetchScalarGridSpec(
                num_scalar_prefetch=1,
                grid=(pairs,),
                in_specs=[window(at), k_spec, v_spec, row, table, table, q_spec, q_spec, window(at)],
                out_specs=[
                    q_spec,
                    k_spec,
                    k_spec,
                    pl.BlockSpec((1, 8, HEAD_SIZE), lambda j, s: (j, 0, 0)),
                ],
                scratch_shapes=[pltpu.VMEM((2, tall, HEAD_SIZE), F32)],
            ),
            out_shape=[
                jax.ShapeDtypeStruct((span, q_width), BF),
                jax.ShapeDtypeStruct((length, kv_width), BF),
                jax.ShapeDtypeStruct((length, kv_width), BF),
                jax.ShapeDtypeStruct((pairs, 8, HEAD_SIZE), F32),
            ],
            compiler_params=params,
            cost_estimate=SMALL,
            name="attention_backward",
        )(seen, q_lin, kv, kv, gain, cosine, sine, o, inv, d)

    return forward, backward


def make_keys(seqs, span, n_kv):
    kv_width = n_kv * HEAD_SIZE

    def forward_kernel(v_ref, gain_ref, cos_ref, sin_ref, o_ref):
        gain = gain_ref[...]
        cosine = cos_ref[...]
        sine = sin_ref[...]
        out = []
        for g in range(n_kv):
            v = v_ref[:, g * HEAD_SIZE : (g + 1) * HEAD_SIZE]
            n = v * lax.rsqrt(jnp.mean(v * v, axis=1, keepdims=True) + EPS) * gain
            out.append(n * cosine + turn(n) * sine)
        o_ref[:, :kv_width] = jnp.concatenate(out, axis=1).astype(BF)
        o_ref[:, kv_width:] = v_ref[:, kv_width:].astype(BF)

    def backward_kernel(v_ref, d_ref, gain_ref, cos_ref, sin_ref, o_ref, dg_ref):
        gain = gain_ref[...]
        cosine = cos_ref[...]
        sine = sin_ref[...]
        out = []
        total = jnp.zeros((span, HEAD_SIZE), F32)
        for g in range(n_kv):
            v = v_ref[:, g * HEAD_SIZE : (g + 1) * HEAD_SIZE]
            d = d_ref[:, g * HEAD_SIZE : (g + 1) * HEAD_SIZE]
            inv = lax.rsqrt(jnp.mean(v * v, axis=1, keepdims=True) + EPS)
            e = d * cosine + turn_back(d * sine)
            scaled = e * gain
            out.append(inv * scaled - v * inv**3 * jnp.mean(scaled * v, axis=1, keepdims=True))
            total = total + e * v * inv
        o_ref[:, :kv_width] = jnp.concatenate(out, axis=1).astype(BF)
        o_ref[:, kv_width:] = d_ref[:, kv_width:].astype(BF)
        dg_ref[...] = jnp.broadcast_to(jnp.sum(total, axis=0, keepdims=True), (8, HEAD_SIZE))

    row = pl.BlockSpec((1, HEAD_SIZE), lambda i: (0, 0))
    table = pl.BlockSpec((span, HEAD_SIZE), lambda i: (0, 0))
    params = pltpu.CompilerParams(dimension_semantics=("arbitrary",))

    def window(at):
        return pl.BlockSpec((span, 2 * kv_width), lambda i: (at, 0))

    def forward(at, lin, gain, cosine, sine):
        return pl.pallas_call(
            forward_kernel,
            grid=(1,),
            in_specs=[window(at), row, table, table],
            out_specs=window(0),
            out_shape=jax.ShapeDtypeStruct((span, 2 * kv_width), BF),
            compiler_params=params,
            cost_estimate=SMALL,
            name="key_forward",
        )(lin, gain, cosine, sine)

    def backward(at, lin, d, gain, cosine, sine):
        return pl.pallas_call(
            backward_kernel,
            grid=(1,),
            in_specs=[window(at), window(0), row, table, table],
            out_specs=[window(0), pl.BlockSpec((8, HEAD_SIZE), lambda i: (0, 0))],
            out_shape=[
                jax.ShapeDtypeStruct((span, 2 * kv_width), BF),
                jax.ShapeDtypeStruct((8, HEAD_SIZE), F32),
            ],
            compiler_params=params,
            cost_estimate=SMALL,
            name="key_backward",
        )(lin, d, gain, cosine, sine)

    return forward, backward


def two_gradients(n, dg, du):
    tokens, width = n.shape
    part = dg.shape[1]
    unit = 256

    def kernel(n_ref, dg_ref, du_ref, gate_ref, up_ref):
        v = n_ref[...]
        gate_ref[...] = dot(v, dg_ref[...], TN).astype(BF)
        up_ref[...] = dot(v, du_ref[...], TN).astype(BF)

    whole = pl.BlockSpec((tokens, part), lambda i: (0, 0))
    out = pl.BlockSpec((unit, part), lambda i: (i, 0))
    return pl.pallas_call(
        kernel,
        grid=(width // unit,),
        in_specs=[pl.BlockSpec((tokens, unit), lambda i: (0, i)), whole, whole],
        out_specs=[out, out],
        out_shape=[jax.ShapeDtypeStruct((width, part), BF)] * 2,
        compiler_params=pltpu.CompilerParams(dimension_semantics=("arbitrary",)),
        cost_estimate=SMALL,
        name="two_gradients",
    )(n, dg, du)


def mm(left, right):
    return dot(left, right, NN)


def mm_tn(left, right):
    return dot(left, right, TN)


def mm_nt(left, right):
    return dot(left, right, NT)


def rms_norm(v, gain):
    inverse = lax.rsqrt(jnp.mean(v * v, axis=-1, keepdims=True) + EPS)
    return v * inverse * gain, inverse


def rms_back(v, inverse, gain, grad):
    scaled = grad * gain
    back = inverse * scaled - v * inverse**3 * jnp.mean(scaled * v, axis=-1, keepdims=True)
    return back, grad * v * inverse


def tie(*values):
    return lax.optimization_barrier(values)


def make_body(n_line, n_plane):
    n_inner = n_line * 2
    n_tp = 4
    n_group = n_line * n_plane
    n_dev = n_group * n_tp

    def flip(v, axis, size, bit):
        return lax.ppermute(v, axis, [(i, i ^ bit) for i in range(size)])

    def core_swap(v):
        return flip(v, "core", 2, 1)

    def pair_swap(v):
        return flip(v, "pair", 2, 1)

    def by_source(pieces, here):
        held = jnp.stack(pieces)
        shape = held.shape
        bit = 1
        while bit < len(pieces):
            split = held.reshape((-1, 2, bit) + shape[1:])
            turned = jnp.concatenate([split[:, 1:], split[:, :1]], axis=1)
            held = jnp.where((here & bit) != 0, turned, split).reshape(shape)
            bit *= 2
        return held

    def exchange(piece_of, axes, size, here):
        pieces = [piece_of(here)]
        pieces += [flip(piece_of(here ^ b), axes, size, b) for b in range(1, size)]
        return pieces

    def gather_inner(v, here):
        held = v[None]
        bit = n_inner // 2
        while bit:
            other = flip(held, INNER, n_inner, bit)
            high = (here & bit) != 0
            pair = jnp.stack([jnp.where(high, other, held), jnp.where(high, held, other)], axis=1)
            held = pair.reshape((-1,) + v.shape)
            bit //= 2
        return held

    def scatter_inner(v, here):
        held = v
        bit = 1
        while bit < n_inner:
            pair = held.reshape((held.shape[0] // 2, 2) + v.shape[1:])
            high = ((here & bit) != 0).astype(jnp.int32)
            keep = lax.dynamic_index_in_dim(pair, high, 1, keepdims=False)
            send = lax.dynamic_index_in_dim(pair, 1 - high, 1, keepdims=False)
            other = flip(send, INNER, n_inner, bit)
            held = keep.astype(F32) + other.astype(F32)
            bit *= 2
            if bit < n_inner:
                held = held.astype(BF)
        return held[0].astype(F32)

    def sum_pieces(part, axes, size, here):
        pieces = exchange(
            lambda k: lax.dynamic_index_in_dim(part, k, 0, keepdims=False), axes, size, here
        )
        total = pieces[0].astype(F32)
        for piece in pieces[1:]:
            total = total + piece.astype(F32)
        return total

    def spread_line(rows, line):
        return by_source(exchange(lambda k: rows, "line", n_line, line), line)

    def whole_rows(held, width):
        return lax.all_gather(held, "plane", axis=1, tiled=True).reshape(-1, width)

    def scatter_plane(whole, lead):
        r = whole.shape[0] // (lead * n_plane)
        if r % 16:
            held = whole.reshape(lead, n_plane, r, whole.shape[1])
            return lax.psum_scatter(held, "plane", scatter_dimension=1)
        held = whole.reshape(lead, n_plane * r, whole.shape[1])
        return lax.psum_scatter(held, "plane", scatter_dimension=1, tiled=True)

    def butterfly_sum(v):
        for axis, size in (("core", 2), ("pair", 2), ("plane", n_plane), ("line", n_line)):
            bit = 1
            while bit < size:
                v = v + flip(v, axis, size, bit)
                bit *= 2
        return v

    def both_cores(v):
        return jnp.concatenate([v, core_swap(v)])

    def fold(partial):
        half = partial.shape[0] // 2
        return partial[:half] + core_swap(partial[half:].astype(BF)).astype(F32)

    def body(x_in, attn_gain, w_query, w_key, w_value, qk_gain, w_out, ffn_gain, w_gate, w_up, w_down, dy_in):
        line = lax.axis_index("line")
        core = lax.axis_index("core")
        here = line * 2 + lax.axis_index("pair")
        tp = lax.axis_index("pair") * 2 + core
        flat = (here * n_plane + lax.axis_index("plane")) * 2 + core
        seqs, span, width = x_in.shape
        rows = seqs * span
        groups = QUERY_HEADS // KEY_VALUE_HEADS
        length = span * n_inner
        q_width = w_query.shape[1]
        kv_width = w_key.shape[1]
        per = w_query.shape[0]
        part = w_gate.shape[1] // n_tp

        def column_part(w):
            pieces = exchange(
                lambda k: lax.dynamic_slice_in_dim(w, k * part, part, axis=1), TP, n_tp, tp
            )
            return by_source(pieces, tp).reshape(2, 2 * per, part)

        def holder(s):
            quarter, group = divmod(s, n_group)
            at_line, at_plane = divmod(group, n_plane)
            return ((at_line * 2 + quarter // 2) * n_plane + at_plane) * 2 + quarter % 2

        spread = [(s, holder(s)) for s in range(n_dev)]
        extra = jnp.zeros((per, 128), BF)
        extra = extra.at[:, 0].set(attn_gain).at[:, 1].set(ffn_gain)
        extra = extra.at[: qk_gain.shape[0], 2].set(qk_gain)
        at_gain = 2 * kv_width
        at_query = at_gain + 128
        at_out = at_query + q_width
        out_rows = jnp.pad(w_out, ((0, per - w_out.shape[0]), (0, 0)))
        packed = jnp.concatenate([w_key, w_value, extra, w_query, out_rows], axis=1)
        packed = lax.all_gather(packed, ALL, axis=0, tiled=True)
        wg = whole_rows(spread_line(column_part(w_gate), line).reshape(n_inner, 2 * per, part), part)
        cut_up = column_part(w_up)
        packed, w_down = tie(packed, w_down)
        cut_down = lax.ppermute(w_down, ALL, spread)
        wkv = packed[:, :at_gain]
        wq = packed[:, at_query:at_out]
        wo = packed[:, at_out:].reshape(n_dev, per, width)[:, : w_out.shape[0]].reshape(-1, width)
        tail = packed[:, at_gain : at_gain + 3].astype(F32)
        g_one = tail[:, 0]
        g_two = tail[:, 1]
        g_qk = tail[:, 2].reshape(n_dev, per)[:, : qk_gain.shape[0]].reshape(-1)
        g_query, g_key = g_qk[:HEAD_SIZE], g_qk[HEAD_SIZE:]

        base = here * span
        positions = (base + jnp.arange(span)).astype(F32)
        freq = 10000.0 ** (-jnp.arange(HEAD_SIZE // 2, dtype=F32) * 2.0 / HEAD_SIZE)
        angle = positions[:, None] * freq[None, :]
        cosine = jnp.concatenate([jnp.cos(angle), jnp.cos(angle)], axis=-1)
        sine = jnp.concatenate([jnp.sin(angle), jnp.sin(angle)], axis=-1)
        unit = min(BLOCK, length)
        seen = ((base // BLOCK + 1) * (BLOCK // unit)).astype(jnp.int32).reshape(1)
        attend, attend_back = make_attention(span, length, KEY_VALUE_HEADS, groups, unit)
        gain_row = g_query.reshape(1, HEAD_SIZE)

        x = x_in.reshape(rows, width).astype(F32)
        normed, inv_one = rms_norm(x, g_one)
        normed_b = normed.astype(BF)
        kv_lin = mm(normed_b, wkv)
        gain_key = g_key.reshape(1, HEAD_SIZE)
        make_key, make_key_back = make_keys(seqs, span, KEY_VALUE_HEADS)
        kv = [make_key(s, kv_lin, gain_key, cosine, sine) for s in range(seqs)]
        gathered = [gather_inner(v, here).reshape(length, 2 * kv_width) for v in kv]
        q_lin = mm(normed_b, wq)
        gathered[0], cut_up = tie(gathered[0], cut_up)
        gathered[-1], cut_down, dy_in = tie(gathered[-1], cut_down, dy_in)
        dy = dy_in.reshape(rows, width)
        dy_far = pair_swap(dy)
        cut_down = spread_line(cut_down, line)
        wu = whole_rows(spread_line(cut_up, line).reshape(n_inner, 2 * per, part), part)
        kept = []
        resids = []
        invs = []
        n2s = []
        for s in range(seqs):
            o, total = attend(s, seen, q_lin, gathered[s], gain_row, cosine, sine)
            if s == seqs - 1:
                o, cut_down, dy_far = tie(o, cut_down, dy_far)
                wd = whole_rows(cut_down, width)
            kept.append((o, total))
            resid = x[s * span : (s + 1) * span] + mm(o, wo)
            normed2, inv_two = rms_norm(resid, g_two)
            resids.append(resid)
            invs.append(inv_two)
            n2s.append(normed2.astype(BF))
        mixed = jnp.concatenate([o for o, _ in kept])
        resid = jnp.concatenate(resids)
        inv_two = jnp.concatenate(invs)
        n2_near = both_cores(jnp.concatenate(n2s))
        far = [pair_swap(v) for v in n2s]

        def expand(n2):
            gate = mm(n2, wg)
            up = mm(n2, wu)
            return gate, up, (gate * jax.nn.sigmoid(gate) * up).astype(BF)

        def expand_back(dy, gate, up):
            d_hidden = mm_nt(dy, wd)
            sigma = jax.nn.sigmoid(gate)
            dg = (d_hidden * up * (sigma * (1.0 + gate * (1.0 - sigma)))).astype(BF)
            return dg, (d_hidden * (gate * sigma)).astype(BF)

        gate_near, up_near, hidden_near = expand(n2_near)
        hidden_near, *far = tie(hidden_near, *far)
        n2_far = both_cores(jnp.concatenate(far))
        gate_far, up_far, hidden_far = expand(n2_far)
        hidden = jnp.concatenate([hidden_near, hidden_far])
        n2_all = jnp.concatenate([n2_near, n2_far])

        dy_near = both_cores(dy)
        dy_far = both_cores(dy_far)
        grad_down = mm_tn(hidden, jnp.concatenate([dy_near, dy_far])).astype(BF)
        wd, grad_down = tie(wd, grad_down)
        down_part = scatter_plane(grad_down, n_line)
        dg_far, du_far = expand_back(dy_far, gate_far, up_far)
        sent = fold(mm_nt(dg_far, wg) + mm_nt(du_far, wu)).astype(BF)
        sent, dy_near = tie(sent, dy_near)
        dg_near, du_near = expand_back(dy_near, gate_near, up_near)
        dn2 = fold(mm_nt(dg_near, wg) + mm_nt(du_near, wu))
        grad_gate, grad_up = two_gradients(
            n2_all, jnp.concatenate([dg_near, dg_far]), jnp.concatenate([du_near, du_far])
        )
        got = pair_swap(sent)
        gate_part = scatter_plane(grad_gate, n_inner)
        up_part = scatter_plane(grad_up, n_inner)
        dn2, hidden_near, hidden_far = tie(dn2, hidden_near, hidden_far)
        sent_out = fold(mm(hidden_far, wd)).astype(BF)
        kept_out = fold(mm(hidden_near, wd))
        got, dn2, grad_gate, grad_up, down_part, sent_out, kept_out = tie(
            got, dn2, grad_gate, grad_up, down_part, sent_out, kept_out
        )
        down_sum = sum_pieces(down_part, "line", n_line, line).astype(BF)
        dn2 = dn2 + got.astype(F32)
        back_two, terms_two = rms_back(resid, inv_two, g_two, dn2)
        grad_gain_two = jnp.sum(terms_two, axis=0)
        d_resid = dy.astype(F32) + back_two

        def column_whole(piece):
            held = piece.astype(BF)
            pieces = exchange(
                lambda k: lax.dynamic_index_in_dim(held, k, 0, keepdims=False), TP, n_tp, tp
            )
            return by_source(pieces, tp).transpose(1, 0, 2).reshape(per, -1).astype(F32)

        def fold_core(whole):
            r = whole.shape[0] // n_dev
            held = whole.reshape(n_dev // 2, 2, r, -1)
            mine = lax.dynamic_index_in_dim(held, core, 1, keepdims=False)
            got = core_swap(lax.dynamic_index_in_dim(held, 1 - core, 1, keepdims=False))
            held = (mine.astype(F32) + got.astype(F32)).astype(BF)
            return held.reshape(whole.shape[0] // 2, -1)

        drb = d_resid.astype(BF)
        dm = mm_nt(drb, wo).astype(BF)
        out_part = scatter_plane(fold_core(mm_tn(mixed, drb).astype(BF)), n_inner)
        output = resid + (kept_out + pair_swap(sent_out).astype(F32))
        dm, down_sum, gate_part, up_part = tie(dm, down_sum, gate_part, up_part)
        gate_sum = sum_pieces(gate_part.reshape(n_line, n_tp, per, part), "line", n_line, line)
        up_sum = sum_pieces(up_part.reshape(n_line, n_tp, per, part), "line", n_line, line)
        dq = []
        dkv = []
        gains_q = []
        for s in range(seqs):
            dq_s, dk_s, dv_s, dg_s = attend_back(
                s, seen, q_lin, gathered[s], gain_row, cosine, sine, *kept[s], dm
            )
            dq.append(dq_s)
            gains_q.append(jnp.sum(dg_s[:, 0], axis=0))
            both = jnp.concatenate([dk_s, dv_s], axis=1)
            if s == seqs - 1:
                both, gate_sum, up_sum, output = tie(both, gate_sum, up_sum, output)
            dkv.append(scatter_inner(both.reshape(n_inner, span, 2 * kv_width), here))
        d_down = lax.ppermute(down_sum, ALL, [(b, a) for a, b in spread]).astype(F32)
        result = output.astype(BF).reshape(seqs, span, width)
        dkv[-1], out_part = tie(dkv[-1], out_part)
        d_out = sum_pieces(out_part, INNER, n_inner, here)
        d_kvs = []
        gains_k = []
        for s in range(seqs):
            d_kv_s, dg_s = make_key_back(s, kv_lin, dkv[s], gain_key, cosine, sine)
            d_kvs.append(d_kv_s)
            gains_k.append(dg_s[0])
        grad_qk = jnp.concatenate([sum(gains_q), sum(gains_k)])
        d_lin = jnp.concatenate([jnp.concatenate(dq), jnp.concatenate(d_kvs)], axis=1)
        grad_qkv = mm_tn(normed_b, d_lin).astype(BF)
        qkv_part = scatter_plane(fold_core(grad_qkv), n_inner)
        d_lin, grad_qkv, d_out = tie(d_lin, grad_qkv, d_out)
        d_gate = column_whole(gate_sum)
        d_up = column_whole(up_sum)
        dn = mm_nt(d_lin[:, :q_width], wq) + mm_nt(d_lin[:, q_width:], wkv)
        back_one, terms_one = rms_back(x, inv_one, g_one, dn)
        grad_gain_one = jnp.sum(terms_one, axis=0)
        d_inputs = (d_resid + back_one).reshape(seqs, span, width)

        gains = butterfly_sum(jnp.concatenate([grad_gain_one, grad_gain_two, grad_qk]))
        d_qkv = sum_pieces(qkv_part, INNER, n_inner, here)
        d_attn_gain = lax.dynamic_slice_in_dim(gains, flat * per, per)
        d_ffn_gain = lax.dynamic_slice_in_dim(gains, width + flat * per, per)
        n_qk = qk_gain.shape[0]
        d_qk = lax.dynamic_slice_in_dim(gains, 2 * width + flat * n_qk, n_qk)
        return (
            result,
            d_inputs,
            d_attn_gain,
            d_qkv[:, :q_width],
            d_qkv[:, q_width : q_width + kv_width],
            d_qkv[:, q_width + kv_width :],
            d_qk,
            d_out,
            d_ffn_gain,
            d_gate,
            d_up,
            d_down,
        )

    return body


def solution(mesh):
    n_line = mesh.shape["inner"] // 2
    n_plane = mesh.shape["outer"] // 2
    fine = Mesh(mesh.devices.reshape(n_line, 2, n_plane, 2), ALL)
    tokens = P(("plane", "core"), INNER, None)
    vec = P(ALL)
    mat = P(ALL, None)
    return jax.shard_map(
        make_body(n_line, n_plane),
        mesh=fine,
        in_specs=(tokens, vec, mat, mat, mat, vec, mat, vec, mat, mat, mat, tokens),
        out_specs=(tokens, tokens, vec, mat, mat, mat, vec, mat, vec, mat, mat, mat),
        check_vma=False,
    )
```

```python
import jax
import jax.numpy as jnp
from jax import lax
from jax.experimental import pallas as pl
from jax.experimental.pallas import tpu as pltpu
from jax.sharding import Mesh, PartitionSpec as P

QUERY_HEADS = 24
KEY_VALUE_HEADS = 6
HEAD_SIZE = 64
BLOCK = 256
EPS = 1e-06
LOG2E = 1.4426950408889634
TP = ("pair", "core")
INNER = ("line", "pair")
ALL = ("line", "pair", "plane", "core")
BF = jnp.bfloat16
F32 = jnp.float32
SMALL = pl.CostEstimate(flops=1000, transcendentals=0, bytes_accessed=1000)


NT = (((1,), (1,)), ((), ()))
NN = (((1,), (0,)), ((), ()))
TN = (((0,), (0,)), ((), ()))


def dot(a, b, dims):
    return lax.dot_general(a, b, dims, preferred_element_type=F32)


def turn(v):
    half = HEAD_SIZE // 2
    return jnp.concatenate([-v[:, half:], v[:, :half]], axis=1)


def turn_back(v):
    half = HEAD_SIZE // 2
    return jnp.concatenate([v[:, half:], -v[:, :half]], axis=1)


def make_attention(span, length, n_kv, groups, unit):
    pairs = n_kv // 2
    wide = 2 * groups * HEAD_SIZE
    scale = HEAD_SIZE ** (-0.5)
    tall = groups * span

    def queries(q_ref, gain, cosine, sine, g):
        out = []
        for h in range(groups):
            at = (g * groups + h) * HEAD_SIZE
            v = q_ref[:, at : at + HEAD_SIZE]
            inv = lax.rsqrt(jnp.mean(v * v, axis=1, keepdims=True) + EPS)
            n = v * inv * gain
            out.append(((n * cosine + turn(n) * sine) * (scale * LOG2E)).astype(BF))
        return jnp.concatenate(out, axis=0)

    def forward_kernel(seen_ref, q_ref, k_ref, v_ref, gain_ref, cos_ref, sin_ref, o_ref, l_ref):
        gain = gain_ref[...]
        cosine = cos_ref[...]
        sine = sin_ref[...]
        ones = jnp.ones((unit, HEAD_SIZE), BF)
        q_all = [queries(q_ref, gain, cosine, sine, g) for g in range(2)]

        def step(i, accs):
            at = pl.ds(pl.multiple_of(i * unit, unit), unit)
            out = []
            for g in range(2):
                lanes = slice(g * HEAD_SIZE, (g + 1) * HEAD_SIZE)
                k = k_ref[at, :][:, lanes]
                v = jnp.concatenate([v_ref[at, :][:, lanes], ones], axis=1)
                e = jnp.exp2(dot(q_all[g], k, NT)).astype(BF)
                out.append(accs[g] + dot(e, v, NN))
            return tuple(out)

        zero = jnp.zeros((tall, 2 * HEAD_SIZE), F32)
        accs = lax.fori_loop(0, seen_ref[0], step, (zero, zero))
        for g in range(2):
            inv = 1.0 / accs[g][:, HEAD_SIZE:]
            o = (accs[g][:, :HEAD_SIZE] * inv).astype(BF)
            for h in range(groups):
                at = (g * groups + h) * HEAD_SIZE
                o_ref[:, at : at + HEAD_SIZE] = o[h * span : (h + 1) * span]
                l_ref[:, at : at + HEAD_SIZE] = inv[h * span : (h + 1) * span]

    def backward_kernel(
        seen_ref, q_ref, k_ref, v_ref, gain_ref, cos_ref, sin_ref, o_ref, l_ref, d_ref,
        dq_ref, dk_ref, dv_ref, dg_ref, acc_ref,
    ):
        gain = gain_ref[...]
        cosine = cos_ref[...]
        sine = sin_ref[...]
        ones = jnp.ones((unit, HEAD_SIZE), BF)
        q_all = []
        d_all = []
        d_aug = []
        for g in range(2):
            q_all.append(queries(q_ref, gain, cosine, sine, g))
            rows = []
            more = []
            for h in range(groups):
                at = (g * groups + h) * HEAD_SIZE
                d = d_ref[:, at : at + HEAD_SIZE].astype(F32)
                inv = l_ref[:, at : at + HEAD_SIZE]
                o = o_ref[:, at : at + HEAD_SIZE].astype(F32)
                delta = -jnp.sum(d * o, axis=1, keepdims=True) * inv
                top = delta.astype(BF)
                low = (delta - top.astype(F32)).astype(BF)
                lane = lax.broadcasted_iota(jnp.int32, (span, HEAD_SIZE), 1)
                side = jnp.where(lane == 0, top.astype(F32), jnp.where(lane == 1, low.astype(F32), 0.0))
                rows.append((d * inv).astype(BF))
                more.append(side.astype(BF))
            d_all.append(jnp.concatenate(rows, axis=0))
            d_aug.append(jnp.concatenate([d_all[g], jnp.concatenate(more, axis=0)], axis=1))
        acc_ref[...] = jnp.zeros_like(acc_ref)
        dk_ref[...] = jnp.zeros_like(dk_ref)
        dv_ref[...] = jnp.zeros_like(dv_ref)

        def step(i, carry):
            at = pl.ds(pl.multiple_of(i * unit, unit), unit)
            dk = []
            dv = []
            for g in range(2):
                lanes = slice(g * HEAD_SIZE, (g + 1) * HEAD_SIZE)
                k = k_ref[at, :][:, lanes]
                v = jnp.concatenate([v_ref[at, :][:, lanes], ones], axis=1)
                e = jnp.exp2(dot(k, q_all[g], NT))
                ds = (e * dot(v, d_aug[g], NT)).astype(BF)
                dv.append(dot(e.astype(BF), d_all[g], NN))
                dk.append(dot(ds, q_all[g], NN))
                acc_ref[g] += dot(ds, k, TN)
            dk_ref[at, :] = (jnp.concatenate(dk, axis=1) * (1.0 / LOG2E)).astype(BF)
            dv_ref[at, :] = jnp.concatenate(dv, axis=1).astype(BF)
            return carry

        lax.fori_loop(0, seen_ref[0], step, 0)
        total = jnp.zeros((span, HEAD_SIZE), F32)
        for g in range(2):
            for h in range(groups):
                at = (g * groups + h) * HEAD_SIZE
                dr = acc_ref[g, h * span : (h + 1) * span, :] * scale
                v = q_ref[:, at : at + HEAD_SIZE]
                inv = lax.rsqrt(jnp.mean(v * v, axis=1, keepdims=True) + EPS)
                e = dr * cosine + turn_back(dr * sine)
                scaled = e * gain
                back = inv * scaled - v * inv**3 * jnp.mean(scaled * v, axis=1, keepdims=True)
                total = total + e * v * inv
                dq_ref[:, at : at + HEAD_SIZE] = back.astype(BF)
        dg_ref[0] = jnp.broadcast_to(jnp.sum(total, axis=0, keepdims=True), (8, HEAD_SIZE))

    def window(at):
        return pl.BlockSpec((span, wide), lambda j, s: (at, j))

    q_spec = window(0)
    k_spec = pl.BlockSpec((length, 2 * HEAD_SIZE), lambda j, s: (0, j))
    v_spec = pl.BlockSpec((length, 2 * HEAD_SIZE), lambda j, s: (0, pairs + j))
    row = pl.BlockSpec((1, HEAD_SIZE), lambda j, s: (0, 0))
    table = pl.BlockSpec((span, HEAD_SIZE), lambda j, s: (0, 0))
    q_width = pairs * wide
    kv_width = n_kv * HEAD_SIZE
    params = pltpu.CompilerParams(dimension_semantics=("arbitrary",))

    def forward(at, seen, q_lin, kv, gain, cosine, sine):
        return pl.pallas_call(
            forward_kernel,
            grid_spec=pltpu.PrefetchScalarGridSpec(
                num_scalar_prefetch=1,
                grid=(pairs,),
                in_specs=[window(at), k_spec, v_spec, row, table, table],
                out_specs=[q_spec, q_spec],
            ),
            out_shape=[
                jax.ShapeDtypeStruct((span, q_width), BF),
                jax.ShapeDtypeStruct((span, q_width), F32),
            ],
            compiler_params=params,
            cost_estimate=SMALL,
            name="attention_forward",
        )(seen, q_lin, kv, kv, gain, cosine, sine)

    def backward(at, seen, q_lin, kv, gain, cosine, sine, o, inv, d):
        return pl.pallas_call(
            backward_kernel,
            grid_spec=pltpu.PrefetchScalarGridSpec(
                num_scalar_prefetch=1,
                grid=(pairs,),
                in_specs=[window(at), k_spec, v_spec, row, table, table, q_spec, q_spec, window(at)],
                out_specs=[
                    q_spec,
                    k_spec,
                    k_spec,
                    pl.BlockSpec((1, 8, HEAD_SIZE), lambda j, s: (j, 0, 0)),
                ],
                scratch_shapes=[pltpu.VMEM((2, tall, HEAD_SIZE), F32)],
            ),
            out_shape=[
                jax.ShapeDtypeStruct((span, q_width), BF),
                jax.ShapeDtypeStruct((length, kv_width), BF),
                jax.ShapeDtypeStruct((length, kv_width), BF),
                jax.ShapeDtypeStruct((pairs, 8, HEAD_SIZE), F32),
            ],
            compiler_params=params,
            cost_estimate=SMALL,
            name="attention_backward",
        )(seen, q_lin, kv, kv, gain, cosine, sine, o, inv, d)

    return forward, backward


def make_keys(seqs, span, n_kv):
    kv_width = n_kv * HEAD_SIZE

    def forward_kernel(v_ref, gain_ref, cos_ref, sin_ref, o_ref):
        gain = gain_ref[...]
        cosine = cos_ref[...]
        sine = sin_ref[...]
        out = []
        for g in range(n_kv):
            v = v_ref[:, g * HEAD_SIZE : (g + 1) * HEAD_SIZE]
            n = v * lax.rsqrt(jnp.mean(v * v, axis=1, keepdims=True) + EPS) * gain
            out.append(n * cosine + turn(n) * sine)
        o_ref[:, :kv_width] = jnp.concatenate(out, axis=1).astype(BF)
        o_ref[:, kv_width:] = v_ref[:, kv_width:].astype(BF)

    def backward_kernel(v_ref, d_ref, gain_ref, cos_ref, sin_ref, o_ref, dg_ref):
        gain = gain_ref[...]
        cosine = cos_ref[...]
        sine = sin_ref[...]
        out = []
        total = jnp.zeros((span, HEAD_SIZE), F32)
        for g in range(n_kv):
            v = v_ref[:, g * HEAD_SIZE : (g + 1) * HEAD_SIZE]
            d = d_ref[:, g * HEAD_SIZE : (g + 1) * HEAD_SIZE]
            inv = lax.rsqrt(jnp.mean(v * v, axis=1, keepdims=True) + EPS)
            e = d * cosine + turn_back(d * sine)
            scaled = e * gain
            out.append(inv * scaled - v * inv**3 * jnp.mean(scaled * v, axis=1, keepdims=True))
            total = total + e * v * inv
        o_ref[:, :kv_width] = jnp.concatenate(out, axis=1).astype(BF)
        o_ref[:, kv_width:] = d_ref[:, kv_width:].astype(BF)
        dg_ref[...] = jnp.broadcast_to(jnp.sum(total, axis=0, keepdims=True), (8, HEAD_SIZE))

    row = pl.BlockSpec((1, HEAD_SIZE), lambda i: (0, 0))
    table = pl.BlockSpec((span, HEAD_SIZE), lambda i: (0, 0))
    params = pltpu.CompilerParams(dimension_semantics=("arbitrary",))

    def window(at):
        return pl.BlockSpec((span, 2 * kv_width), lambda i: (at, 0))

    def forward(at, lin, gain, cosine, sine):
        return pl.pallas_call(
            forward_kernel,
            grid=(1,),
            in_specs=[window(at), row, table, table],
            out_specs=window(0),
            out_shape=jax.ShapeDtypeStruct((span, 2 * kv_width), BF),
            compiler_params=params,
            cost_estimate=SMALL,
            name="key_forward",
        )(lin, gain, cosine, sine)

    def backward(at, lin, d, gain, cosine, sine):
        return pl.pallas_call(
            backward_kernel,
            grid=(1,),
            in_specs=[window(at), window(0), row, table, table],
            out_specs=[window(0), pl.BlockSpec((8, HEAD_SIZE), lambda i: (0, 0))],
            out_shape=[
                jax.ShapeDtypeStruct((span, 2 * kv_width), BF),
                jax.ShapeDtypeStruct((8, HEAD_SIZE), F32),
            ],
            compiler_params=params,
            cost_estimate=SMALL,
            name="key_backward",
        )(lin, d, gain, cosine, sine)

    return forward, backward


def two_gradients(n, dg, du):
    tokens, width = n.shape
    part = dg.shape[1]
    unit = 256

    def kernel(n_ref, dg_ref, du_ref, gate_ref, up_ref):
        v = n_ref[...]
        gate_ref[...] = dot(v, dg_ref[...], TN).astype(BF)
        up_ref[...] = dot(v, du_ref[...], TN).astype(BF)

    whole = pl.BlockSpec((tokens, part), lambda i: (0, 0))
    out = pl.BlockSpec((unit, part), lambda i: (i, 0))
    return pl.pallas_call(
        kernel,
        grid=(width // unit,),
        in_specs=[pl.BlockSpec((tokens, unit), lambda i: (0, i)), whole, whole],
        out_specs=[out, out],
        out_shape=[jax.ShapeDtypeStruct((width, part), BF)] * 2,
        compiler_params=pltpu.CompilerParams(dimension_semantics=("arbitrary",)),
        cost_estimate=SMALL,
        name="two_gradients",
    )(n, dg, du)


def mm(left, right):
    return dot(left, right, NN)


def mm_tn(left, right):
    return dot(left, right, TN)


def mm_nt(left, right):
    return dot(left, right, NT)


def rms_norm(v, gain):
    inverse = lax.rsqrt(jnp.mean(v * v, axis=-1, keepdims=True) + EPS)
    return v * inverse * gain, inverse


def rms_back(v, inverse, gain, grad):
    scaled = grad * gain
    back = inverse * scaled - v * inverse**3 * jnp.mean(scaled * v, axis=-1, keepdims=True)
    return back, grad * v * inverse


def tie(*values):
    return lax.optimization_barrier(values)


def make_body(n_line, n_plane):
    n_inner = n_line * 2
    n_tp = 4
    n_group = n_line * n_plane
    n_dev = n_group * n_tp

    def flip(v, axis, size, bit):
        return lax.ppermute(v, axis, [(i, i ^ bit) for i in range(size)])

    def core_swap(v):
        return flip(v, "core", 2, 1)

    def pair_swap(v):
        return flip(v, "pair", 2, 1)

    def by_source(pieces, here):
        held = jnp.stack(pieces)
        shape = held.shape
        bit = 1
        while bit < len(pieces):
            split = held.reshape((-1, 2, bit) + shape[1:])
            turned = jnp.concatenate([split[:, 1:], split[:, :1]], axis=1)
            held = jnp.where((here & bit) != 0, turned, split).reshape(shape)
            bit *= 2
        return held

    def exchange(piece_of, axes, size, here):
        pieces = [piece_of(here)]
        pieces += [flip(piece_of(here ^ b), axes, size, b) for b in range(1, size)]
        return pieces

    def gather_inner(v, here):
        held = v[None]
        bit = n_inner // 2
        while bit:
            other = flip(held, INNER, n_inner, bit)
            high = (here & bit) != 0
            pair = jnp.stack([jnp.where(high, other, held), jnp.where(high, held, other)], axis=1)
            held = pair.reshape((-1,) + v.shape)
            bit //= 2
        return held

    def scatter_inner(v, here):
        held = v
        bit = 1
        while bit < n_inner:
            pair = held.reshape((held.shape[0] // 2, 2) + v.shape[1:])
            high = ((here & bit) != 0).astype(jnp.int32)
            keep = lax.dynamic_index_in_dim(pair, high, 1, keepdims=False)
            send = lax.dynamic_index_in_dim(pair, 1 - high, 1, keepdims=False)
            other = flip(send, INNER, n_inner, bit)
            held = keep.astype(F32) + other.astype(F32)
            bit *= 2
            if bit < n_inner:
                held = held.astype(BF)
        return held[0].astype(F32)

    def sum_pieces(part, axes, size, here):
        pieces = exchange(
            lambda k: lax.dynamic_index_in_dim(part, k, 0, keepdims=False), axes, size, here
        )
        total = pieces[0].astype(F32)
        for piece in pieces[1:]:
            total = total + piece.astype(F32)
        return total

    def spread_line(rows, line):
        return by_source(exchange(lambda k: rows, "line", n_line, line), line)

    def whole_rows(held, width):
        return lax.all_gather(held, "plane", axis=1, tiled=True).reshape(-1, width)

    def scatter_plane(whole, lead):
        r = whole.shape[0] // (lead * n_plane)
        if r % 16:
            held = whole.reshape(lead, n_plane, r, whole.shape[1])
            return lax.psum_scatter(held, "plane", scatter_dimension=1)
        held = whole.reshape(lead, n_plane * r, whole.shape[1])
        return lax.psum_scatter(held, "plane", scatter_dimension=1, tiled=True)

    def butterfly_sum(v):
        for axis, size in (("core", 2), ("pair", 2), ("plane", n_plane), ("line", n_line)):
            bit = 1
            while bit < size:
                v = v + flip(v, axis, size, bit)
                bit *= 2
        return v

    def both_cores(v):
        return jnp.concatenate([v, core_swap(v)])

    def fold(partial):
        half = partial.shape[0] // 2
        return partial[:half] + core_swap(partial[half:].astype(BF)).astype(F32)

    def body(x_in, attn_gain, w_query, w_key, w_value, qk_gain, w_out, ffn_gain, w_gate, w_up, w_down, dy_in):
        line = lax.axis_index("line")
        core = lax.axis_index("core")
        here = line * 2 + lax.axis_index("pair")
        tp = lax.axis_index("pair") * 2 + core
        flat = (here * n_plane + lax.axis_index("plane")) * 2 + core
        seqs, span, width = x_in.shape
        rows = seqs * span
        groups = QUERY_HEADS // KEY_VALUE_HEADS
        length = span * n_inner
        q_width = w_query.shape[1]
        kv_width = w_key.shape[1]
        per = w_query.shape[0]
        part = w_gate.shape[1] // n_tp

        def column_part(w):
            pieces = exchange(
                lambda k: lax.dynamic_slice_in_dim(w, k * part, part, axis=1), TP, n_tp, tp
            )
            return by_source(pieces, tp).reshape(2, 2 * per, part)

        def holder(s):
            quarter, group = divmod(s, n_group)
            at_line, at_plane = divmod(group, n_plane)
            return ((at_line * 2 + quarter // 2) * n_plane + at_plane) * 2 + quarter % 2

        spread = [(s, holder(s)) for s in range(n_dev)]
        extra = jnp.zeros((per, 128), BF)
        extra = extra.at[:, 0].set(attn_gain).at[:, 1].set(ffn_gain)
        extra = extra.at[: qk_gain.shape[0], 2].set(qk_gain)
        at_gain = 2 * kv_width
        at_query = at_gain + 128
        at_out = at_query + q_width
        out_rows = jnp.pad(w_out, ((0, per - w_out.shape[0]), (0, 0)))
        packed = jnp.concatenate([w_key, w_value, extra, w_query, out_rows], axis=1)
        packed = lax.all_gather(packed, ALL, axis=0, tiled=True)
        wg = whole_rows(spread_line(column_part(w_gate), line).reshape(n_inner, 2 * per, part), part)
        cut_up = column_part(w_up)
        dy = dy_in.reshape(rows, width)
        packed, w_down, cut_up, dy_far = tie(packed, w_down, cut_up, pair_swap(dy))
        cut_down = lax.ppermute(w_down, ALL, spread)
        wkv = packed[:, :at_gain]
        wq = packed[:, at_query:at_out]
        wo = packed[:, at_out:].reshape(n_dev, per, width)[:, : w_out.shape[0]].reshape(-1, width)
        tail = packed[:, at_gain : at_gain + 3].astype(F32)
        g_one = tail[:, 0]
        g_two = tail[:, 1]
        g_qk = tail[:, 2].reshape(n_dev, per)[:, : qk_gain.shape[0]].reshape(-1)
        g_query, g_key = g_qk[:HEAD_SIZE], g_qk[HEAD_SIZE:]

        base = here * span
        positions = (base + jnp.arange(span)).astype(F32)
        freq = 10000.0 ** (-jnp.arange(HEAD_SIZE // 2, dtype=F32) * 2.0 / HEAD_SIZE)
        angle = positions[:, None] * freq[None, :]
        cosine = jnp.concatenate([jnp.cos(angle), jnp.cos(angle)], axis=-1)
        sine = jnp.concatenate([jnp.sin(angle), jnp.sin(angle)], axis=-1)
        unit = min(BLOCK, length)
        seen = ((base // BLOCK + 1) * (BLOCK // unit)).astype(jnp.int32).reshape(1)
        attend, attend_back = make_attention(span, length, KEY_VALUE_HEADS, groups, unit)
        gain_row = g_query.reshape(1, HEAD_SIZE)

        x = x_in.reshape(rows, width).astype(F32)
        normed, inv_one = rms_norm(x, g_one)
        normed_b = normed.astype(BF)
        kv_lin = mm(normed_b, wkv)
        gain_key = g_key.reshape(1, HEAD_SIZE)
        make_key, make_key_back = make_keys(seqs, span, KEY_VALUE_HEADS)
        kv = [make_key(s, kv_lin, gain_key, cosine, sine) for s in range(seqs)]
        gathered = [gather_inner(v, here).reshape(length, 2 * kv_width) for v in kv]
        q_lin = mm(normed_b, wq)
        gathered[-1], cut_down = tie(gathered[-1], cut_down)
        cut_down = spread_line(cut_down, line)
        wu = whole_rows(spread_line(cut_up, line).reshape(n_inner, 2 * per, part), part)
        kept = []
        resids = []
        invs = []
        n2s = []
        for s in range(seqs):
            o, total = attend(s, seen, q_lin, gathered[s], gain_row, cosine, sine)
            if s == seqs - 1:
                o, cut_down = tie(o, cut_down)
                wd = whole_rows(cut_down, width)
            kept.append((o, total))
            resid = x[s * span : (s + 1) * span] + mm(o, wo)
            normed2, inv_two = rms_norm(resid, g_two)
            resids.append(resid)
            invs.append(inv_two)
            n2s.append(normed2.astype(BF))
        mixed = jnp.concatenate([o for o, _ in kept])
        resid = jnp.concatenate(resids)
        inv_two = jnp.concatenate(invs)
        n2_near = both_cores(jnp.concatenate(n2s))
        far = [pair_swap(v) for v in n2s]

        def expand(n2):
            gate = mm(n2, wg)
            up = mm(n2, wu)
            return gate, up, (gate * jax.nn.sigmoid(gate) * up).astype(BF)

        def expand_back(dy, gate, up):
            d_hidden = mm_nt(dy, wd)
            sigma = jax.nn.sigmoid(gate)
            dg = (d_hidden * up * (sigma * (1.0 + gate * (1.0 - sigma)))).astype(BF)
            return dg, (d_hidden * (gate * sigma)).astype(BF)

        gate_near, up_near, hidden_near = expand(n2_near)
        hidden_near, *far = tie(hidden_near, *far)
        n2_far = both_cores(jnp.concatenate(far))
        gate_far, up_far, hidden_far = expand(n2_far)
        hidden = jnp.concatenate([hidden_near, hidden_far])
        n2_all = jnp.concatenate([n2_near, n2_far])

        dy_near = both_cores(dy)
        dy_far = both_cores(dy_far)
        grad_down = mm_tn(hidden, jnp.concatenate([dy_near, dy_far])).astype(BF)
        wd, grad_down = tie(wd, grad_down)
        down_part = scatter_plane(grad_down, n_line)
        dg_far, du_far = expand_back(dy_far, gate_far, up_far)
        sent = fold(mm_nt(dg_far, wg) + mm_nt(du_far, wu)).astype(BF)
        sent, dy_near = tie(sent, dy_near)
        dg_near, du_near = expand_back(dy_near, gate_near, up_near)
        grad_gate, grad_up = two_gradients(
            n2_all, jnp.concatenate([dg_near, dg_far]), jnp.concatenate([du_near, du_far])
        )
        got, dg_near, du_near, grad_gate, grad_up = tie(pair_swap(sent), dg_near, du_near, grad_gate, grad_up)
        dn2 = fold(mm_nt(dg_near, wg) + mm_nt(du_near, wu))
        gate_part = scatter_plane(grad_gate, n_inner)
        up_part = scatter_plane(grad_up, n_inner)
        dn2, hidden_near, hidden_far = tie(dn2, hidden_near, hidden_far)
        sent_out = fold(mm(hidden_far, wd)).astype(BF)
        kept_out = fold(mm(hidden_near, wd))
        dn2, down_part, sent_out, kept_out = tie(dn2, down_part, sent_out, kept_out)
        down_sum = sum_pieces(down_part, "line", n_line, line).astype(BF)
        dn2 = dn2 + got.astype(F32)
        back_two, terms_two = rms_back(resid, inv_two, g_two, dn2)
        grad_gain_two = jnp.sum(terms_two, axis=0)
        d_resid = dy.astype(F32) + back_two

        def column_whole(piece):
            held = piece.astype(BF)
            pieces = exchange(
                lambda k: lax.dynamic_index_in_dim(held, k, 0, keepdims=False), TP, n_tp, tp
            )
            return by_source(pieces, tp).transpose(1, 0, 2).reshape(per, -1).astype(F32)

        def fold_core(whole):
            r = whole.shape[0] // n_dev
            held = whole.reshape(n_dev // 2, 2, r, -1)
            mine = lax.dynamic_index_in_dim(held, core, 1, keepdims=False)
            got = core_swap(lax.dynamic_index_in_dim(held, 1 - core, 1, keepdims=False))
            held = (mine.astype(F32) + got.astype(F32)).astype(BF)
            return held.reshape(whole.shape[0] // 2, -1)

        drb = d_resid.astype(BF)
        dm = mm_nt(drb, wo).astype(BF)
        out_part = scatter_plane(fold_core(mm_tn(mixed, drb).astype(BF)), n_inner)
        dm, gate_part = tie(dm, gate_part)
        gate_sum = sum_pieces(gate_part.reshape(n_line, n_tp, per, part), "line", n_line, line)
        dq = []
        dkv = []
        gains_q = []
        for s in range(seqs):
            dq_s, dk_s, dv_s, dg_s = attend_back(
                s, seen, q_lin, gathered[s], gain_row, cosine, sine, *kept[s], dm
            )
            dq.append(dq_s)
            gains_q.append(jnp.sum(dg_s[:, 0], axis=0))
            both = jnp.concatenate([dk_s, dv_s], axis=1)
            if s == seqs - 1:
                both, gate_sum, down_sum = tie(both, gate_sum, down_sum)
            dkv.append(scatter_inner(both.reshape(n_inner, span, 2 * kv_width), here))
        d_down = lax.ppermute(down_sum, ALL, [(b, a) for a, b in spread]).astype(F32)
        dkv[-1], out_part, up_part, sent_out = tie(dkv[-1], out_part, up_part, sent_out)
        output = resid + (kept_out + pair_swap(sent_out).astype(F32))
        up_sum = sum_pieces(up_part.reshape(n_line, n_tp, per, part), "line", n_line, line)
        d_out = sum_pieces(out_part, INNER, n_inner, here)
        d_kvs = []
        gains_k = []
        for s in range(seqs):
            d_kv_s, dg_s = make_key_back(s, kv_lin, dkv[s], gain_key, cosine, sine)
            d_kvs.append(d_kv_s)
            gains_k.append(dg_s[0])
        grad_qk = jnp.concatenate([sum(gains_q), sum(gains_k)])
        d_lin = jnp.concatenate([jnp.concatenate(dq), jnp.concatenate(d_kvs)], axis=1)
        grad_qkv = mm_tn(normed_b, d_lin).astype(BF)
        qkv_part = scatter_plane(fold_core(grad_qkv), n_inner)
        d_lin, grad_qkv, d_out, up_sum, output = tie(d_lin, grad_qkv, d_out, up_sum, output)
        result = output.astype(BF).reshape(seqs, span, width)
        d_gate = column_whole(gate_sum)
        d_up = column_whole(up_sum)
        dn = mm_nt(d_lin[:, :q_width], wq) + mm_nt(d_lin[:, q_width:], wkv)
        back_one, terms_one = rms_back(x, inv_one, g_one, dn)
        grad_gain_one = jnp.sum(terms_one, axis=0)
        d_inputs = (d_resid + back_one).reshape(seqs, span, width)

        gains = butterfly_sum(jnp.concatenate([grad_gain_one, grad_gain_two, grad_qk]))
        d_qkv = sum_pieces(qkv_part, INNER, n_inner, here)
        d_attn_gain = lax.dynamic_slice_in_dim(gains, flat * per, per)
        d_ffn_gain = lax.dynamic_slice_in_dim(gains, width + flat * per, per)
        n_qk = qk_gain.shape[0]
        d_qk = lax.dynamic_slice_in_dim(gains, 2 * width + flat * n_qk, n_qk)
        return (
            result,
            d_inputs,
            d_attn_gain,
            d_qkv[:, :q_width],
            d_qkv[:, q_width : q_width + kv_width],
            d_qkv[:, q_width + kv_width :],
            d_qk,
            d_out,
            d_ffn_gain,
            d_gate,
            d_up,
            d_down,
        )

    return body


def solution(mesh):
    n_line = mesh.shape["inner"] // 2
    n_plane = mesh.shape["outer"] // 2
    fine = Mesh(mesh.devices.reshape(n_line, 2, n_plane, 2), ALL)
    tokens = P(("plane", "core"), INNER, None)
    vec = P(ALL)
    mat = P(ALL, None)
    return jax.shard_map(
        make_body(n_line, n_plane),
        mesh=fine,
        in_specs=(tokens, vec, mat, mat, mat, vec, mat, vec, mat, mat, mat, tokens),
        out_specs=(tokens, tokens, vec, mat, mat, mat, vec, mat, vec, mat, mat, mat),
        check_vma=False,
    )
```

```python
import jax
import jax.numpy as jnp
from jax import lax
from jax.experimental import pallas as pl
from jax.experimental.pallas import tpu as pltpu
from jax.sharding import Mesh, PartitionSpec as P

QUERY_HEADS = 24
KEY_VALUE_HEADS = 6
HEAD_SIZE = 64
BLOCK = 256
EPS = 1e-06
LOG2E = 1.4426950408889634
TP = ("pair", "core")
INNER = ("line", "pair")
ALL = ("line", "pair", "plane", "core")
BF = jnp.bfloat16
F32 = jnp.float32
SMALL = pl.CostEstimate(flops=1000, transcendentals=0, bytes_accessed=1000)


NT = (((1,), (1,)), ((), ()))
NN = (((1,), (0,)), ((), ()))
TN = (((0,), (0,)), ((), ()))


def dot(a, b, dims):
    return lax.dot_general(a, b, dims, preferred_element_type=F32)


def turn(v):
    half = HEAD_SIZE // 2
    return jnp.concatenate([-v[:, half:], v[:, :half]], axis=1)


def turn_back(v):
    half = HEAD_SIZE // 2
    return jnp.concatenate([v[:, half:], -v[:, :half]], axis=1)


def make_attention(span, length, n_kv, groups, unit):
    pairs = n_kv // 2
    wide = 2 * groups * HEAD_SIZE
    scale = HEAD_SIZE ** (-0.5)
    tall = groups * span

    def queries(q_ref, gain, cosine, sine, g):
        out = []
        for h in range(groups):
            at = (g * groups + h) * HEAD_SIZE
            v = q_ref[:, at : at + HEAD_SIZE]
            inv = lax.rsqrt(jnp.mean(v * v, axis=1, keepdims=True) + EPS)
            n = v * inv * gain
            out.append(((n * cosine + turn(n) * sine) * (scale * LOG2E)).astype(BF))
        return jnp.concatenate(out, axis=0)

    def forward_kernel(seen_ref, q_ref, k_ref, v_ref, gain_ref, cos_ref, sin_ref, o_ref, l_ref):
        gain = gain_ref[...]
        cosine = cos_ref[...]
        sine = sin_ref[...]
        ones = jnp.ones((unit, HEAD_SIZE), BF)
        q_all = [queries(q_ref, gain, cosine, sine, g) for g in range(2)]

        def step(i, accs):
            at = pl.ds(pl.multiple_of(i * unit, unit), unit)
            out = []
            for g in range(2):
                lanes = slice(g * HEAD_SIZE, (g + 1) * HEAD_SIZE)
                k = k_ref[at, :][:, lanes]
                v = jnp.concatenate([v_ref[at, :][:, lanes], ones], axis=1)
                e = jnp.exp2(dot(q_all[g], k, NT)).astype(BF)
                out.append(accs[g] + dot(e, v, NN))
            return tuple(out)

        zero = jnp.zeros((tall, 2 * HEAD_SIZE), F32)
        accs = lax.fori_loop(0, seen_ref[0], step, (zero, zero))
        for g in range(2):
            inv = 1.0 / accs[g][:, HEAD_SIZE:]
            o = (accs[g][:, :HEAD_SIZE] * inv).astype(BF)
            for h in range(groups):
                at = (g * groups + h) * HEAD_SIZE
                o_ref[:, at : at + HEAD_SIZE] = o[h * span : (h + 1) * span]
                l_ref[:, at : at + HEAD_SIZE] = inv[h * span : (h + 1) * span]

    def backward_kernel(
        seen_ref, q_ref, k_ref, v_ref, gain_ref, cos_ref, sin_ref, o_ref, l_ref, d_ref,
        dq_ref, dk_ref, dv_ref, dg_ref, acc_ref,
    ):
        gain = gain_ref[...]
        cosine = cos_ref[...]
        sine = sin_ref[...]
        ones = jnp.ones((unit, HEAD_SIZE), BF)
        q_all = []
        d_all = []
        d_aug = []
        for g in range(2):
            q_all.append(queries(q_ref, gain, cosine, sine, g))
            rows = []
            more = []
            for h in range(groups):
                at = (g * groups + h) * HEAD_SIZE
                d = d_ref[:, at : at + HEAD_SIZE].astype(F32)
                inv = l_ref[:, at : at + HEAD_SIZE]
                o = o_ref[:, at : at + HEAD_SIZE].astype(F32)
                delta = -jnp.sum(d * o, axis=1, keepdims=True) * inv
                top = delta.astype(BF)
                low = (delta - top.astype(F32)).astype(BF)
                lane = lax.broadcasted_iota(jnp.int32, (span, HEAD_SIZE), 1)
                side = jnp.where(lane == 0, top.astype(F32), jnp.where(lane == 1, low.astype(F32), 0.0))
                rows.append((d * inv).astype(BF))
                more.append(side.astype(BF))
            d_all.append(jnp.concatenate(rows, axis=0))
            d_aug.append(jnp.concatenate([d_all[g], jnp.concatenate(more, axis=0)], axis=1))
        acc_ref[...] = jnp.zeros_like(acc_ref)
        dk_ref[...] = jnp.zeros_like(dk_ref)
        dv_ref[...] = jnp.zeros_like(dv_ref)

        def step(i, carry):
            at = pl.ds(pl.multiple_of(i * unit, unit), unit)
            dk = []
            dv = []
            for g in range(2):
                lanes = slice(g * HEAD_SIZE, (g + 1) * HEAD_SIZE)
                k = k_ref[at, :][:, lanes]
                v = jnp.concatenate([v_ref[at, :][:, lanes], ones], axis=1)
                e = jnp.exp2(dot(k, q_all[g], NT))
                ds = (e * dot(v, d_aug[g], NT)).astype(BF)
                dv.append(dot(e.astype(BF), d_all[g], NN))
                dk.append(dot(ds, q_all[g], NN))
                acc_ref[g] += dot(ds, k, TN)
            dk_ref[at, :] = (jnp.concatenate(dk, axis=1) * (1.0 / LOG2E)).astype(BF)
            dv_ref[at, :] = jnp.concatenate(dv, axis=1).astype(BF)
            return carry

        lax.fori_loop(0, seen_ref[0], step, 0)
        total = jnp.zeros((span, HEAD_SIZE), F32)
        for g in range(2):
            for h in range(groups):
                at = (g * groups + h) * HEAD_SIZE
                dr = acc_ref[g, h * span : (h + 1) * span, :] * scale
                v = q_ref[:, at : at + HEAD_SIZE]
                inv = lax.rsqrt(jnp.mean(v * v, axis=1, keepdims=True) + EPS)
                e = dr * cosine + turn_back(dr * sine)
                scaled = e * gain
                back = inv * scaled - v * inv**3 * jnp.mean(scaled * v, axis=1, keepdims=True)
                total = total + e * v * inv
                dq_ref[:, at : at + HEAD_SIZE] = back.astype(BF)
        dg_ref[0] = jnp.broadcast_to(jnp.sum(total, axis=0, keepdims=True), (8, HEAD_SIZE))

    def window(at):
        return pl.BlockSpec((span, wide), lambda j, s: (at, j))

    q_spec = window(0)
    k_spec = pl.BlockSpec((length, 2 * HEAD_SIZE), lambda j, s: (0, j))
    v_spec = pl.BlockSpec((length, 2 * HEAD_SIZE), lambda j, s: (0, pairs + j))
    row = pl.BlockSpec((1, HEAD_SIZE), lambda j, s: (0, 0))
    table = pl.BlockSpec((span, HEAD_SIZE), lambda j, s: (0, 0))
    q_width = pairs * wide
    kv_width = n_kv * HEAD_SIZE
    params = pltpu.CompilerParams(dimension_semantics=("arbitrary",))

    def forward(at, seen, q_lin, kv, gain, cosine, sine):
        return pl.pallas_call(
            forward_kernel,
            grid_spec=pltpu.PrefetchScalarGridSpec(
                num_scalar_prefetch=1,
                grid=(pairs,),
                in_specs=[window(at), k_spec, v_spec, row, table, table],
                out_specs=[q_spec, q_spec],
            ),
            out_shape=[
                jax.ShapeDtypeStruct((span, q_width), BF),
                jax.ShapeDtypeStruct((span, q_width), F32),
            ],
            compiler_params=params,
            cost_estimate=SMALL,
            name="attention_forward",
        )(seen, q_lin, kv, kv, gain, cosine, sine)

    def backward(at, seen, q_lin, kv, gain, cosine, sine, o, inv, d):
        return pl.pallas_call(
            backward_kernel,
            grid_spec=pltpu.PrefetchScalarGridSpec(
                num_scalar_prefetch=1,
                grid=(pairs,),
                in_specs=[window(at), k_spec, v_spec, row, table, table, q_spec, q_spec, window(at)],
                out_specs=[
                    q_spec,
                    k_spec,
                    k_spec,
                    pl.BlockSpec((1, 8, HEAD_SIZE), lambda j, s: (j, 0, 0)),
                ],
                scratch_shapes=[pltpu.VMEM((2, tall, HEAD_SIZE), F32)],
            ),
            out_shape=[
                jax.ShapeDtypeStruct((span, q_width), BF),
                jax.ShapeDtypeStruct((length, kv_width), BF),
                jax.ShapeDtypeStruct((length, kv_width), BF),
                jax.ShapeDtypeStruct((pairs, 8, HEAD_SIZE), F32),
            ],
            compiler_params=params,
            cost_estimate=SMALL,
            name="attention_backward",
        )(seen, q_lin, kv, kv, gain, cosine, sine, o, inv, d)

    return forward, backward


def make_keys(seqs, span, n_kv):
    kv_width = n_kv * HEAD_SIZE

    def forward_kernel(v_ref, gain_ref, cos_ref, sin_ref, o_ref):
        gain = gain_ref[...]
        cosine = cos_ref[...]
        sine = sin_ref[...]
        out = []
        for g in range(n_kv):
            v = v_ref[:, g * HEAD_SIZE : (g + 1) * HEAD_SIZE]
            n = v * lax.rsqrt(jnp.mean(v * v, axis=1, keepdims=True) + EPS) * gain
            out.append(n * cosine + turn(n) * sine)
        o_ref[:, :kv_width] = jnp.concatenate(out, axis=1).astype(BF)
        o_ref[:, kv_width:] = v_ref[:, kv_width:].astype(BF)

    def backward_kernel(v_ref, d_ref, gain_ref, cos_ref, sin_ref, o_ref, dg_ref):
        gain = gain_ref[...]
        cosine = cos_ref[...]
        sine = sin_ref[...]
        out = []
        total = jnp.zeros((span, HEAD_SIZE), F32)
        for g in range(n_kv):
            v = v_ref[:, g * HEAD_SIZE : (g + 1) * HEAD_SIZE]
            d = d_ref[:, g * HEAD_SIZE : (g + 1) * HEAD_SIZE]
            inv = lax.rsqrt(jnp.mean(v * v, axis=1, keepdims=True) + EPS)
            e = d * cosine + turn_back(d * sine)
            scaled = e * gain
            out.append(inv * scaled - v * inv**3 * jnp.mean(scaled * v, axis=1, keepdims=True))
            total = total + e * v * inv
        o_ref[:, :kv_width] = jnp.concatenate(out, axis=1).astype(BF)
        o_ref[:, kv_width:] = d_ref[:, kv_width:].astype(BF)
        dg_ref[...] = jnp.broadcast_to(jnp.sum(total, axis=0, keepdims=True), (8, HEAD_SIZE))

    row = pl.BlockSpec((1, HEAD_SIZE), lambda i: (0, 0))
    table = pl.BlockSpec((span, HEAD_SIZE), lambda i: (0, 0))
    params = pltpu.CompilerParams(dimension_semantics=("arbitrary",))

    def window(at):
        return pl.BlockSpec((span, 2 * kv_width), lambda i: (at, 0))

    def forward(at, lin, gain, cosine, sine):
        return pl.pallas_call(
            forward_kernel,
            grid=(1,),
            in_specs=[window(at), row, table, table],
            out_specs=window(0),
            out_shape=jax.ShapeDtypeStruct((span, 2 * kv_width), BF),
            compiler_params=params,
            cost_estimate=SMALL,
            name="key_forward",
        )(lin, gain, cosine, sine)

    def backward(at, lin, d, gain, cosine, sine):
        return pl.pallas_call(
            backward_kernel,
            grid=(1,),
            in_specs=[window(at), window(0), row, table, table],
            out_specs=[window(0), pl.BlockSpec((8, HEAD_SIZE), lambda i: (0, 0))],
            out_shape=[
                jax.ShapeDtypeStruct((span, 2 * kv_width), BF),
                jax.ShapeDtypeStruct((8, HEAD_SIZE), F32),
            ],
            compiler_params=params,
            cost_estimate=SMALL,
            name="key_backward",
        )(lin, d, gain, cosine, sine)

    return forward, backward


def two_gradients(n, dg, du):
    tokens, width = n.shape
    part = dg.shape[1]
    unit = 256

    def kernel(n_ref, dg_ref, du_ref, gate_ref, up_ref):
        v = n_ref[...]
        gate_ref[...] = dot(v, dg_ref[...], TN).astype(BF)
        up_ref[...] = dot(v, du_ref[...], TN).astype(BF)

    whole = pl.BlockSpec((tokens, part), lambda i: (0, 0))
    out = pl.BlockSpec((unit, part), lambda i: (i, 0))
    return pl.pallas_call(
        kernel,
        grid=(width // unit,),
        in_specs=[pl.BlockSpec((tokens, unit), lambda i: (0, i)), whole, whole],
        out_specs=[out, out],
        out_shape=[jax.ShapeDtypeStruct((width, part), BF)] * 2,
        compiler_params=pltpu.CompilerParams(dimension_semantics=("arbitrary",)),
        cost_estimate=SMALL,
        name="two_gradients",
    )(n, dg, du)


def mm(left, right):
    return dot(left, right, NN)


def mm_tn(left, right):
    return dot(left, right, TN)


def mm_nt(left, right):
    return dot(left, right, NT)


def rms_norm(v, gain):
    inverse = lax.rsqrt(jnp.mean(v * v, axis=-1, keepdims=True) + EPS)
    return v * inverse * gain, inverse


def rms_back(v, inverse, gain, grad):
    scaled = grad * gain
    back = inverse * scaled - v * inverse**3 * jnp.mean(scaled * v, axis=-1, keepdims=True)
    return back, grad * v * inverse


def tie(*values):
    return lax.optimization_barrier(values)


def make_body(n_line, n_plane):
    n_inner = n_line * 2
    n_tp = 4
    n_group = n_line * n_plane
    n_dev = n_group * n_tp

    def flip(v, axis, size, bit):
        return lax.ppermute(v, axis, [(i, i ^ bit) for i in range(size)])

    def core_swap(v):
        return flip(v, "core", 2, 1)

    def pair_swap(v):
        return flip(v, "pair", 2, 1)

    def by_source(pieces, here):
        held = jnp.stack(pieces)
        shape = held.shape
        bit = 1
        while bit < len(pieces):
            split = held.reshape((-1, 2, bit) + shape[1:])
            turned = jnp.concatenate([split[:, 1:], split[:, :1]], axis=1)
            held = jnp.where((here & bit) != 0, turned, split).reshape(shape)
            bit *= 2
        return held

    def exchange(piece_of, axes, size, here):
        pieces = [piece_of(here)]
        pieces += [flip(piece_of(here ^ b), axes, size, b) for b in range(1, size)]
        return pieces

    def gather_inner(v, here):
        held = v[None]
        bit = n_inner // 2
        while bit:
            other = flip(held, INNER, n_inner, bit)
            high = (here & bit) != 0
            pair = jnp.stack([jnp.where(high, other, held), jnp.where(high, held, other)], axis=1)
            held = pair.reshape((-1,) + v.shape)
            bit //= 2
        return held

    def scatter_inner(v, here):
        held = v
        bit = 1
        while bit < n_inner:
            pair = held.reshape((held.shape[0] // 2, 2) + v.shape[1:])
            high = ((here & bit) != 0).astype(jnp.int32)
            keep = lax.dynamic_index_in_dim(pair, high, 1, keepdims=False)
            send = lax.dynamic_index_in_dim(pair, 1 - high, 1, keepdims=False)
            other = flip(send, INNER, n_inner, bit)
            held = keep.astype(F32) + other.astype(F32)
            bit *= 2
            if bit < n_inner:
                held = held.astype(BF)
        return held[0].astype(F32)

    def sum_pieces(part, axes, size, here):
        pieces = exchange(
            lambda k: lax.dynamic_index_in_dim(part, k, 0, keepdims=False), axes, size, here
        )
        total = pieces[0].astype(F32)
        for piece in pieces[1:]:
            total = total + piece.astype(F32)
        return total

    def spread_line(rows, line):
        return by_source(exchange(lambda k: rows, "line", n_line, line), line)

    def whole_rows(held, width):
        return lax.all_gather(held, "plane", axis=1, tiled=True).reshape(-1, width)

    def scatter_plane(whole, lead):
        r = whole.shape[0] // (lead * n_plane)
        if r % 16:
            held = whole.reshape(lead, n_plane, r, whole.shape[1])
            return lax.psum_scatter(held, "plane", scatter_dimension=1)
        held = whole.reshape(lead, n_plane * r, whole.shape[1])
        return lax.psum_scatter(held, "plane", scatter_dimension=1, tiled=True)

    def butterfly_sum(v):
        for axis, size in (("core", 2), ("pair", 2), ("plane", n_plane), ("line", n_line)):
            bit = 1
            while bit < size:
                v = v + flip(v, axis, size, bit)
                bit *= 2
        return v

    def both_cores(v):
        return jnp.concatenate([v, core_swap(v)])

    def fold(partial):
        half = partial.shape[0] // 2
        return partial[:half] + core_swap(partial[half:].astype(BF)).astype(F32)

    def body(x_in, attn_gain, w_query, w_key, w_value, qk_gain, w_out, ffn_gain, w_gate, w_up, w_down, dy_in):
        line = lax.axis_index("line")
        core = lax.axis_index("core")
        here = line * 2 + lax.axis_index("pair")
        tp = lax.axis_index("pair") * 2 + core
        flat = (here * n_plane + lax.axis_index("plane")) * 2 + core
        seqs, span, width = x_in.shape
        rows = seqs * span
        groups = QUERY_HEADS // KEY_VALUE_HEADS
        length = span * n_inner
        q_width = w_query.shape[1]
        kv_width = w_key.shape[1]
        per = w_query.shape[0]
        part = w_gate.shape[1] // n_tp

        def column_part(w):
            pieces = exchange(
                lambda k: lax.dynamic_slice_in_dim(w, k * part, part, axis=1), TP, n_tp, tp
            )
            return by_source(pieces, tp).reshape(2, 2 * per, part)

        def holder(s):
            quarter, group = divmod(s, n_group)
            at_line, at_plane = divmod(group, n_plane)
            return ((at_line * 2 + quarter // 2) * n_plane + at_plane) * 2 + quarter % 2

        spread = [(s, holder(s)) for s in range(n_dev)]
        extra = jnp.zeros((per, 128), BF)
        extra = extra.at[:, 0].set(attn_gain).at[:, 1].set(ffn_gain)
        extra = extra.at[: qk_gain.shape[0], 2].set(qk_gain)
        at_gain = 2 * kv_width
        at_query = at_gain + 128
        at_out = at_query + q_width
        out_rows = jnp.pad(w_out, ((0, per - w_out.shape[0]), (0, 0)))
        packed = jnp.concatenate([w_key, w_value, extra, w_query, out_rows], axis=1)
        packed = lax.all_gather(packed, ALL, axis=0, tiled=True)
        wg = whole_rows(spread_line(column_part(w_gate), line).reshape(n_inner, 2 * per, part), part)
        cut_up = column_part(w_up)
        dy = dy_in.reshape(rows, width)
        packed, w_down, cut_up, dy_far = tie(packed, w_down, cut_up, pair_swap(dy))
        cut_down = lax.ppermute(w_down, ALL, spread)
        wkv = packed[:, :at_gain]
        wq = packed[:, at_query:at_out]
        wo = packed[:, at_out:].reshape(n_dev, per, width)[:, : w_out.shape[0]].reshape(-1, width)
        tail = packed[:, at_gain : at_gain + 3].astype(F32)
        g_one = tail[:, 0]
        g_two = tail[:, 1]
        g_qk = tail[:, 2].reshape(n_dev, per)[:, : qk_gain.shape[0]].reshape(-1)
        g_query, g_key = g_qk[:HEAD_SIZE], g_qk[HEAD_SIZE:]

        base = here * span
        positions = (base + jnp.arange(span)).astype(F32)
        freq = 10000.0 ** (-jnp.arange(HEAD_SIZE // 2, dtype=F32) * 2.0 / HEAD_SIZE)
        angle = positions[:, None] * freq[None, :]
        cosine = jnp.concatenate([jnp.cos(angle), jnp.cos(angle)], axis=-1)
        sine = jnp.concatenate([jnp.sin(angle), jnp.sin(angle)], axis=-1)
        unit = min(BLOCK, length)
        seen = ((base // BLOCK + 1) * (BLOCK // unit)).astype(jnp.int32).reshape(1)
        attend, attend_back = make_attention(span, length, KEY_VALUE_HEADS, groups, unit)
        gain_row = g_query.reshape(1, HEAD_SIZE)

        x = x_in.reshape(rows, width).astype(F32)
        normed, inv_one = rms_norm(x, g_one)
        normed_b = normed.astype(BF)
        kv_lin = mm(normed_b, wkv)
        gain_key = g_key.reshape(1, HEAD_SIZE)
        make_key, make_key_back = make_keys(seqs, span, KEY_VALUE_HEADS)
        kv = [make_key(s, kv_lin, gain_key, cosine, sine) for s in range(seqs)]
        gathered = [gather_inner(v, here).reshape(length, 2 * kv_width) for v in kv]
        q_lin = mm(normed_b, wq)
        gathered[0], cut_down = tie(gathered[0], cut_down)
        gathered[-1], cut_down = tie(gathered[-1], cut_down)
        cut_down = spread_line(cut_down, line)
        wu = whole_rows(spread_line(cut_up, line).reshape(n_inner, 2 * per, part), part)
        kept = []
        resids = []
        invs = []
        n2s = []
        for s in range(seqs):
            o, total = attend(s, seen, q_lin, gathered[s], gain_row, cosine, sine)
            if s == seqs - 1:
                o, cut_down = tie(o, cut_down)
                wd = whole_rows(cut_down, width)
            kept.append((o, total))
            resid = x[s * span : (s + 1) * span] + mm(o, wo)
            normed2, inv_two = rms_norm(resid, g_two)
            resids.append(resid)
            invs.append(inv_two)
            n2s.append(normed2.astype(BF))
        mixed = jnp.concatenate([o for o, _ in kept])
        resid = jnp.concatenate(resids)
        inv_two = jnp.concatenate(invs)
        n2_near = both_cores(jnp.concatenate(n2s))
        far = [pair_swap(v) for v in n2s]

        def expand(n2):
            gate = mm(n2, wg)
            up = mm(n2, wu)
            return gate, up, (gate * jax.nn.sigmoid(gate) * up).astype(BF)

        def expand_back(dy, gate, up):
            d_hidden = mm_nt(dy, wd)
            sigma = jax.nn.sigmoid(gate)
            dg = (d_hidden * up * (sigma * (1.0 + gate * (1.0 - sigma)))).astype(BF)
            return dg, (d_hidden * (gate * sigma)).astype(BF)

        gate_near, up_near, hidden_near = expand(n2_near)
        hidden_near, *far = tie(hidden_near, *far)
        n2_far = both_cores(jnp.concatenate(far))
        gate_far, up_far, hidden_far = expand(n2_far)
        hidden = jnp.concatenate([hidden_near, hidden_far])
        n2_all = jnp.concatenate([n2_near, n2_far])

        dy_near = both_cores(dy)
        dy_far = both_cores(dy_far)
        grad_down = mm_tn(hidden, jnp.concatenate([dy_near, dy_far])).astype(BF)
        wd, grad_down = tie(wd, grad_down)
        down_part = scatter_plane(grad_down, n_line)
        dg_far, du_far = expand_back(dy_far, gate_far, up_far)
        sent = fold(mm_nt(dg_far, wg) + mm_nt(du_far, wu)).astype(BF)
        sent, dy_near = tie(sent, dy_near)
        dg_near, du_near = expand_back(dy_near, gate_near, up_near)
        grad_gate, grad_up = two_gradients(
            n2_all, jnp.concatenate([dg_near, dg_far]), jnp.concatenate([du_near, du_far])
        )
        got, dg_near, du_near, grad_gate, grad_up = tie(pair_swap(sent), dg_near, du_near, grad_gate, grad_up)
        dn2 = fold(mm_nt(dg_near, wg) + mm_nt(du_near, wu))
        gate_part = scatter_plane(grad_gate, n_inner)
        up_part = scatter_plane(grad_up, n_inner)
        dn2, hidden_near, hidden_far = tie(dn2, hidden_near, hidden_far)
        sent_out = fold(mm(hidden_far, wd)).astype(BF)
        kept_out = fold(mm(hidden_near, wd))
        dn2, down_part, sent_out, kept_out = tie(dn2, down_part, sent_out, kept_out)
        dn2 = dn2 + got.astype(F32)
        back_two, terms_two = rms_back(resid, inv_two, g_two, dn2)
        grad_gain_two = jnp.sum(terms_two, axis=0)
        d_resid = dy.astype(F32) + back_two

        def column_whole(piece):
            held = piece.astype(BF)
            pieces = exchange(
                lambda k: lax.dynamic_index_in_dim(held, k, 0, keepdims=False), TP, n_tp, tp
            )
            return by_source(pieces, tp).transpose(1, 0, 2).reshape(per, -1).astype(F32)

        def fold_core(whole):
            r = whole.shape[0] // n_dev
            held = whole.reshape(n_dev // 2, 2, r, -1)
            mine = lax.dynamic_index_in_dim(held, core, 1, keepdims=False)
            got = core_swap(lax.dynamic_index_in_dim(held, 1 - core, 1, keepdims=False))
            held = (mine.astype(F32) + got.astype(F32)).astype(BF)
            return held.reshape(whole.shape[0] // 2, -1)

        drb = d_resid.astype(BF)
        dm = mm_nt(drb, wo).astype(BF)
        out_part = scatter_plane(fold_core(mm_tn(mixed, drb).astype(BF)), n_inner)
        dm, gate_part, down_part = tie(dm, gate_part, down_part)
        down_sum = sum_pieces(down_part, "line", n_line, line).astype(BF)
        output = resid + (kept_out + pair_swap(sent_out).astype(F32))
        gate_sum = sum_pieces(gate_part.reshape(n_line, n_tp, per, part), "line", n_line, line)
        dq = []
        dkv = []
        gains_q = []
        for s in range(seqs):
            dq_s, dk_s, dv_s, dg_s = attend_back(
                s, seen, q_lin, gathered[s], gain_row, cosine, sine, *kept[s], dm
            )
            dq.append(dq_s)
            gains_q.append(jnp.sum(dg_s[:, 0], axis=0))
            both = jnp.concatenate([dk_s, dv_s], axis=1)
            if s == seqs - 1:
                both, gate_sum, down_sum, output = tie(both, gate_sum, down_sum, output)
            dkv.append(scatter_inner(both.reshape(n_inner, span, 2 * kv_width), here))
        d_down = lax.ppermute(down_sum, ALL, [(b, a) for a, b in spread]).astype(F32)
        dkv[-1], out_part, up_part = tie(dkv[-1], out_part, up_part)
        up_sum = sum_pieces(up_part.reshape(n_line, n_tp, per, part), "line", n_line, line)
        d_out = sum_pieces(out_part, INNER, n_inner, here)
        d_kvs = []
        gains_k = []
        for s in range(seqs):
            d_kv_s, dg_s = make_key_back(s, kv_lin, dkv[s], gain_key, cosine, sine)
            d_kvs.append(d_kv_s)
            gains_k.append(dg_s[0])
        grad_qk = jnp.concatenate([sum(gains_q), sum(gains_k)])
        d_lin = jnp.concatenate([jnp.concatenate(dq), jnp.concatenate(d_kvs)], axis=1)
        grad_qkv = mm_tn(normed_b, d_lin).astype(BF)
        qkv_part = scatter_plane(fold_core(grad_qkv), n_inner)
        d_lin, grad_qkv, d_out, up_sum = tie(d_lin, grad_qkv, d_out, up_sum)
        result = output.astype(BF).reshape(seqs, span, width)
        d_gate = column_whole(gate_sum)
        d_up = column_whole(up_sum)
        dn = mm_nt(d_lin[:, :q_width], wq) + mm_nt(d_lin[:, q_width:], wkv)
        back_one, terms_one = rms_back(x, inv_one, g_one, dn)
        grad_gain_one = jnp.sum(terms_one, axis=0)
        d_inputs = (d_resid + back_one).reshape(seqs, span, width)

        gains = butterfly_sum(jnp.concatenate([grad_gain_one, grad_gain_two, grad_qk]))
        d_qkv = sum_pieces(qkv_part, INNER, n_inner, here)
        d_attn_gain = lax.dynamic_slice_in_dim(gains, flat * per, per)
        d_ffn_gain = lax.dynamic_slice_in_dim(gains, width + flat * per, per)
        n_qk = qk_gain.shape[0]
        d_qk = lax.dynamic_slice_in_dim(gains, 2 * width + flat * n_qk, n_qk)
        return (
            result,
            d_inputs,
            d_attn_gain,
            d_qkv[:, :q_width],
            d_qkv[:, q_width : q_width + kv_width],
            d_qkv[:, q_width + kv_width :],
            d_qk,
            d_out,
            d_ffn_gain,
            d_gate,
            d_up,
            d_down,
        )

    return body


def solution(mesh):
    n_line = mesh.shape["inner"] // 2
    n_plane = mesh.shape["outer"] // 2
    fine = Mesh(mesh.devices.reshape(n_line, 2, n_plane, 2), ALL)
    tokens = P(("plane", "core"), INNER, None)
    vec = P(ALL)
    mat = P(ALL, None)
    return jax.shard_map(
        make_body(n_line, n_plane),
        mesh=fine,
        in_specs=(tokens, vec, mat, mat, mat, vec, mat, vec, mat, mat, mat, tokens),
        out_specs=(tokens, tokens, vec, mat, mat, mat, vec, mat, vec, mat, mat, mat),
        check_vma=False,
    )
```
